64 devices in a mesh: req: 4 (over x, y), cp: 16 (over z, core).
Axes of the slice: x: 2, y: 2, z: 8, core: 2. Of those that a mesh axis runs over, the one named last changes fastest.
The devices are a block of a 4x4x8 slice.
Arguments:
- x: bfloat16 [16384, 2048], P(('req', 'cp')), parts along dimension 0
- pos: int32 [16384], P(('req', 'cp')), parts along dimension 0
- g1: bfloat16 [2, 2048], replicated
- g2: bfloat16 [2, 2048], replicated
- wq: bfloat16 [2, 2048, 2048], replicated
- wk: bfloat16 [2, 2048, 2048], replicated
- wv: bfloat16 [2, 2048, 2048], replicated
- wo: bfloat16 [2, 2048, 2048], replicated
- w1: bfloat16 [2, 2048, 5504], replicated
- w3: bfloat16 [2, 2048, 5504], replicated
- w2: bfloat16 [2, 5504, 2048], replicated
Outputs:
- output 1: bfloat16 [16384, 2048], P(('req', 'cp')), parts along dimension 0
- output 2: bfloat16 [2, 16384, 16, 128], P(None, 'req', 'cp'), parts along dimension 1
- output 3: bfloat16 [2, 16384, 16, 128], P(None, 'req', 'cp'), parts along dimension 1
There are 4 independent parts. The reference program is written for one: setup_inputs(seed, part) draws one part's arguments, and reference() takes and returns one part's arrays. A program takes and returns all parts, laid end to end along the dimension named above; an argument that names none is the same for every part.
All inputs are finite; a program needn't handle non-finite values.
Results may differ from the reference program's by a relative error of at most 0.0181633.
Values are sent between devices in bfloat16 or wider.
A program may use at most 768 MiB of HBM per device.

```python
import jax
import jax.numpy as jnp
from jax import lax
import numpy as np

D = 2048
HEADS = 16
HEAD = 128
FF = 5504
LAYERS = 2
S_DEV = 256
CP = 16

SEQ = CP * S_DEV
SEG = S_DEV // 2


def _layout():
    rows = [np.arange(c * SEG, (c + 1) * SEG) for i in range(CP) for c in (i, 2 * CP - 1 - i)]
    return np.concatenate(rows).astype(np.int32)


def setup_inputs(seed: int = 0, part: int = 0) -> dict:
    key = jax.random.PRNGKey(seed)
    kx, ko = jax.random.split(jax.random.fold_in(key, part))
    ks = jax.random.split(key, 9)
    hd = HEADS * HEAD

    def w(k, shape, scale):
        return (jax.random.normal(k, shape, jnp.float32) * scale).astype(jnp.bfloat16)

    def gain(k):
        return (1.0 + 0.2 * jax.random.normal(k, (LAYERS, D), jnp.float32)).astype(jnp.bfloat16)

    p0 = jax.random.randint(ko, (), 0, 4096, jnp.int32)
    return {
        "x": jax.random.normal(kx, (SEQ, D), jnp.float32).astype(jnp.bfloat16),
        "pos": p0 + jnp.asarray(_layout()),
        "g1": gain(ks[0]),
        "g2": gain(ks[1]),
        "wq": w(ks[2], (LAYERS, D, hd), 1.7 * D ** -0.5),
        "wk": w(ks[3], (LAYERS, D, hd), 1.7 * D ** -0.5),
        "wv": w(ks[4], (LAYERS, D, hd), D ** -0.5),
        "wo": w(ks[5], (LAYERS, hd, D), hd ** -0.5),
        "w1": w(ks[6], (LAYERS, D, FF), D ** -0.5),
        "w3": w(ks[7], (LAYERS, D, FF), D ** -0.5),
        "w2": w(ks[8], (LAYERS, FF, D), FF ** -0.5),
    }


def _norm(x, g):
    x32 = x.astype(jnp.float32)
    r = lax.rsqrt(jnp.mean(x32 * x32, axis=-1, keepdims=True) + 1e-5)
    return (x32 * r * g.astype(jnp.float32)).astype(jnp.bfloat16)


def _rope(t, pos):
    half = HEAD // 2
    inv = 1.0 / (10000.0 ** (jnp.arange(half, dtype=jnp.float32) * (2.0 / HEAD)))
    ang = pos.astype(jnp.float32)[:, None] * inv[None, :]
    c = jnp.cos(ang)[:, None, :]
    s = jnp.sin(ang)[:, None, :]
    t1, t2 = t[..., :half], t[..., half:]
    return jnp.concatenate([t1 * c - t2 * s, t2 * c + t1 * s], axis=-1)


def _attention(q, k, v, pos):
    nb = SEQ // SEG
    scale = HEAD ** -0.5

    def head(a):
        qh, kh, vh = a

        def blk(b):
            qb, pb = b
            s = jnp.dot(qb, kh.T, preferred_element_type=jnp.float32) * scale
            s = jnp.where(pos[None, :] <= pb[:, None], s, -jnp.inf)
            p = jax.nn.softmax(s, axis=-1).astype(jnp.bfloat16)
            return jnp.dot(p, vh, preferred_element_type=jnp.float32).astype(jnp.bfloat16)

        o = lax.map(blk, (qh.reshape(nb, SEG, HEAD), pos.reshape(nb, SEG)))
        return o.reshape(SEQ, HEAD)

    o = lax.map(head, (q.transpose(1, 0, 2), k.transpose(1, 0, 2), v.transpose(1, 0, 2)))
    return o.transpose(1, 0, 2).reshape(SEQ, HEADS * HEAD)


def reference(x, pos, g1, g2, wq, wk, wv, wo, w1, w3, w2):
    order = jnp.argsort(pos)

    def layer(x, w):
        a1, a2, bq, bk, bv, bo, b1, b3, b2 = w
        h = _norm(x, a1)
        q = _rope(jnp.dot(h, bq, preferred_element_type=jnp.float32).reshape(SEQ, HEADS, HEAD), pos).astype(jnp.bfloat16)
        k = _rope(jnp.dot(h, bk, preferred_element_type=jnp.float32).reshape(SEQ, HEADS, HEAD), pos).astype(jnp.bfloat16)
        v = jnp.dot(h, bv, preferred_element_type=jnp.float32).astype(jnp.bfloat16).reshape(SEQ, HEADS, HEAD)
        o = _attention(q, k, v, pos)
        x = (x.astype(jnp.float32) + jnp.dot(o, bo, preferred_element_type=jnp.float32)).astype(jnp.bfloat16)
        h2 = _norm(x, a2)
        u = (jax.nn.silu(jnp.dot(h2, b1, preferred_element_type=jnp.float32))
             * jnp.dot(h2, b3, preferred_element_type=jnp.float32)).astype(jnp.bfloat16)
        x = (x.astype(jnp.float32) + jnp.dot(u, b2, preferred_element_type=jnp.float32)).astype(jnp.bfloat16)
        return x, (k[order], v[order])

    y, (kc, vc) = lax.scan(layer, x, (g1, g2, wq, wk, wv, wo, w1, w3, w2))
    return y, kc, vc
```

```python
import functools

import jax
import jax.numpy as jnp
from jax import lax
from jax.experimental import pallas as pl
from jax.experimental.pallas import tpu as pltpu
from jax.sharding import PartitionSpec as P

HEAD = 128
F32 = jnp.float32
BF16 = jnp.bfloat16
MESH = pl.DeviceIdType.MESH
CORES = 2
QB = 512
KB = 512
FB = 512
SLOTS = 3
SCALE2 = HEAD ** -0.5 * 1.4426950408889634


def _angles(pos):
    half = HEAD // 2
    inv = 1.0 / (10000.0 ** (jnp.arange(half, dtype=F32) * (2.0 / HEAD)))
    ang = pos.astype(F32)[:, None] * inv
    c, sn = jnp.cos(ang), jnp.sin(ang)
    return jnp.concatenate([c, c], axis=-1), jnp.concatenate([-sn, sn], axis=-1)


def _kernel(ncp, x_ref, cos_ref, sin_ref, g1_ref, g2_ref, wq, wk, wv, wo, w1, w3, w2,
            y_ref, kc_ref, vc_ref,
            x_s, h_s, stage, qkv, o_s, o_stage, m_s, l_s, acc_s, y_acc,
            wqkv_s, wo_s, w13_s, w2_s, w13t_s, w2t_s,
            send_sem, recv_sem, osend_sem, orecv_sem,
            wqkv_sem, wo_sem, wm_sem, wt_sem, out_sem):
    n_layers = wq.shape[0]
    rows, dim = x_ref.shape
    seg = rows // 2
    nseg = 2 * ncp
    seq = nseg * seg
    half_seq = seq // 2
    ff = w1.shape[2]
    nf = ff // FB
    tail = ff - nf * FB
    nchip = ncp // CORES
    cw = CORES * HEAD
    me = lax.axis_index("cp")
    req = lax.axis_index("req")
    chip, core = me // CORES, me % CORES
    others = (ncp - 1) * seg

    def chip_at(j):
        off = nchip // 2 + (2 * (j % 2) - 1) * ((j + 1) // 2)
        return lax.rem(chip + off + nchip, nchip)

    def wqkv_copies(g):
        l, j = g // nchip, lax.rem(g, nchip)
        slot = lax.rem(g, 2)
        cols = pl.ds(pl.multiple_of(chip_at(j) * cw, cw), cw)
        return [pltpu.make_async_copy(w.at[l, :, cols], wqkv_s.at[slot, t], wqkv_sem.at[slot])
                for t, w in enumerate((wk, wv, wq))]

    def mlp_copies(l, f, slot):
        cols = pl.ds(pl.multiple_of(f * FB, FB), FB)
        return [pltpu.make_async_copy(w1.at[l, :, cols], w13_s.at[slot, 0], wm_sem.at[slot]),
                pltpu.make_async_copy(w3.at[l, :, cols], w13_s.at[slot, 1], wm_sem.at[slot]),
                pltpu.make_async_copy(w2.at[l, cols, :], w2_s.at[slot], wm_sem.at[slot])]

    def tail_copies(l):
        cols = pl.ds(nf * FB, tail)
        return [pltpu.make_async_copy(w1.at[l, :, cols], w13t_s.at[0], wt_sem),
                pltpu.make_async_copy(w3.at[l, :, cols], w13t_s.at[1], wt_sem),
                pltpu.make_async_copy(w2.at[l, cols, :], w2t_s, wt_sem)]

    def wo_copy(l):
        return pltpu.make_async_copy(wo.at[l], wo_s, wo_sem)

    def start(cs):
        for c in cs:
            c.start()

    def wait(cs):
        for c in cs:
            c.wait()

    def remote(src, dst, ssem, rsem, dev):
        return pltpu.make_async_remote_copy(src_ref=src, dst_ref=dst, send_sem=ssem, recv_sem=rsem,
                                            device_id=(req, dev), device_id_type=MESH)

    def norm(g_ref, l):
        blk = 32

        def body(i, _):
            r = pl.ds(pl.multiple_of(i * blk, blk), blk)
            v = x_s[r, :].astype(F32)
            s = lax.rsqrt(jnp.mean(v * v, axis=-1, keepdims=True) + 1e-5)
            h_s[r, :] = (v * s * g_ref[l]).astype(BF16)
            return 0

        lax.fori_loop(0, rows // blk, body, 0)

    start(wqkv_copies(0))
    start(wqkv_copies(1))
    barrier = pltpu.get_barrier_semaphore()

    def sig(i, _):
        pl.semaphore_signal(barrier, inc=1, device_id=(req, lax.rem(me + 1 + i, ncp)), device_id_type=MESH)
        return 0

    lax.fori_loop(0, ncp - 1, sig, 0)
    x_s[...] = x_ref[...]
    cosv, sinv = cos_ref[...], sin_ref[...]
    row_of = (me * seg, (nseg - 1 - me) * seg)

    def piece(l, j, t, hh, half):
        dev = chip_at(j) * CORES + hh
        r = pl.ds(pl.multiple_of(row_of[half], seg), seg)
        return remote(stage.at[j, t, hh, pl.ds(half * seg, seg), :], qkv.at[l, t, r, :],
                      send_sem.at[l, half, t], recv_sem.at[l, half, t], dev)

    def send_chunk(l, j, half):
        for t in range(3):
            for hh in range(CORES):
                piece(l, j, t, hh, half).start()

    def attend(l, qb, kb, st, masked):
        q = qkv[l, 2, pl.ds(pl.multiple_of(qb * QB, QB), QB), :]
        kr = pl.ds(pl.multiple_of(kb * KB, KB), KB)
        s = lax.dot_general(q, qkv[l, 0, kr, :], (((1,), (1,)), ((), ())), preferred_element_type=F32)
        if masked:
            ri = lax.broadcasted_iota(jnp.int32, (QB, KB), 0)
            ci = lax.broadcasted_iota(jnp.int32, (QB, KB), 1)
            s = jnp.where(ci <= ri, s, -jnp.inf)
        m_old = m_s[st]
        m_new = jnp.maximum(m_old, jnp.max(s, axis=1, keepdims=True))
        mc = m_new * SCALE2
        alpha = jnp.exp2(m_old * SCALE2 - mc)
        ps, tot = [], l_s[st] * alpha
        for c in range(KB // 128):
            p = jnp.exp2(s[:, c * 128:(c + 1) * 128] * SCALE2 - mc)
            tot = tot + p
            ps.append(p.astype(BF16))
        m_s[st] = m_new
        l_s[st] = tot
        pv = jnp.dot(jnp.concatenate(ps, axis=1), qkv[l, 1, kr, :], preferred_element_type=F32)
        acc_s[st] = acc_s[st] * alpha + pv

    def attend_init(st):
        m_s[st] = jnp.full((QB, 128), -jnp.inf, F32)
        l_s[st] = jnp.zeros((QB, 128), F32)
        acc_s[st] = jnp.zeros((QB, HEAD), F32)

    my_cols = pl.ds(pl.multiple_of(me * HEAD, HEAD), HEAD)
    nblk = half_seq // QB

    def finish(l, qb, st, half):
        o = (acc_s[st] / jnp.sum(l_s[st], axis=1, keepdims=True)).astype(BF16)
        o_stage[pl.ds(pl.multiple_of(qb * QB, QB), QB), :] = o
        for i in range(QB // seg):
            s_i = qb * (QB // seg) + i
            dev = s_i if half == 0 else nseg - 1 - s_i

            @pl.when(dev == me)
            def _():
                o_s[l, half * seg:(half + 1) * seg, my_cols] = o[i * seg:(i + 1) * seg]

            @pl.when(dev != me)
            def _():
                remote(o_stage.at[pl.ds(pl.multiple_of(s_i * seg, seg), seg), :],
                       o_s.at[l, pl.ds(half * seg, seg), my_cols],
                       osend_sem.at[l, half], orecv_sem.at[l, half], dev).start()

    def bulk(l, t, ssem, rsem):
        r = qkv.at[l, t, pl.ds(0, others), :]
        return remote(r, r, ssem, rsem, me)

    def mlp_step(a, w13, w2c):
        g = jnp.dot(a, w13[0], preferred_element_type=F32)
        u = jnp.dot(a, w13[1], preferred_element_type=F32)
        u = (g * (1.0 / (1.0 + jnp.exp(-g))) * u).astype(BF16)
        return jnp.dot(u, w2c, preferred_element_type=F32)

    def layer(l, _):
        norm(g1_ref, l)

        def proj(j, _):
            g = l * nchip + j
            slot = lax.rem(g, 2)
            wait(wqkv_copies(g))
            a = h_s[...]
            for t in range(3):
                r = jnp.dot(a, wqkv_s[slot, t], preferred_element_type=F32)
                for hh in range(CORES):
                    v = r[:, hh * HEAD:(hh + 1) * HEAD]
                    if t != 1:
                        v = v * cosv + pltpu.roll(v, HEAD // 2, 1) * sinv
                    stage[j, t, hh] = v.astype(BF16)

            @pl.when(g + 2 < nchip * n_layers)
            def _():
                start(wqkv_copies(g + 2))

            @pl.when(j > 0)
            def _():
                @pl.when(g == 1)
                def _():
                    pl.semaphore_wait(barrier, ncp - 1)
                send_chunk(l, j - 1, 0)
            return 0

        lax.fori_loop(0, nchip, proj, 0)
        last = nchip - 1
        for half in range(2):
            for t in range(3):
                piece(l, last, t, 1 - core, half).start()
            if half == 0:
                def sendb(j, _):
                    send_chunk(l, j, 1)
                    return 0
                lax.fori_loop(0, last, sendb, 0)
        for half in range(2):
            for t in range(3):
                qkv[l, t, pl.ds(pl.multiple_of(row_of[half], seg), seg), :] = \
                    stage[last, t, core, half * seg:(half + 1) * seg, :]
        wo_copy(l).start()
        start(tail_copies(l))
        for f in range(SLOTS):
            start(mlp_copies(l, f, f))

        for t in range(3):
            bulk(l, t, send_sem.at[l, 0, t], recv_sem.at[l, 0, t]).wait_recv()

        def blk_a(qb, _):
            attend_init(qb)
            lax.fori_loop(0, qb, lambda kb, _: (attend(l, qb, kb, qb, False), 0)[1], 0)
            attend(l, qb, qb, qb, True)
            finish(l, qb, qb, 0)
            return 0

        lax.fori_loop(0, nblk, blk_a, 0)
        bulk(l, 2, send_sem.at[l, 1, 2], recv_sem.at[l, 1, 2]).wait_recv()

        def blk_b1(i, _):
            attend_init(i)
            lax.fori_loop(0, nblk, lambda kb, _: (attend(l, nblk + i, kb, i, False), 0)[1], 0)
            return 0

        lax.fori_loop(0, nblk, blk_b1, 0)
        for t in range(2):
            bulk(l, t, send_sem.at[l, 1, t], recv_sem.at[l, 1, t]).wait_recv()
        kc_out = pltpu.make_async_copy(qkv.at[l, 0], kc_ref.at[l], out_sem.at[0])
        vc_out = pltpu.make_async_copy(qkv.at[l, 1], vc_ref.at[l], out_sem.at[1])
        kc_out.start()
        vc_out.start()

        def blk_b2(i, _):
            qb = nblk + i
            lax.fori_loop(nblk, qb, lambda kb, _: (attend(l, qb, kb, i, False), 0)[1], 0)
            attend(l, qb, qb, i, True)
            finish(l, qb, i, 1)
            return 0

        lax.fori_loop(0, nblk, blk_b2, 0)
        for half in range(2):
            for t in range(3):
                bulk(l, t, send_sem.at[l, half, t], recv_sem.at[l, half, t]).wait_send()
        wo_copy(l).wait()
        for half in range(2):
            bulk(l, 0, osend_sem.at[l, half], orecv_sem.at[l, half]).wait_recv()

        def out_proj(c, _):
            cols = pl.ds(pl.multiple_of(c * FB, FB), FB)
            x_s[:, cols] = (x_s[:, cols].astype(F32)
                            + jnp.dot(o_s[l], wo_s[:, cols], preferred_element_type=F32)).astype(BF16)
            return 0

        lax.fori_loop(0, dim // FB, out_proj, 0)
        norm(g2_ref, l)
        wait(tail_copies(l))
        y_acc[...] = mlp_step(h_s[...], w13t_s, w2t_s[...])

        def mlp(f, _):
            slot = lax.rem(f, SLOTS)
            wait(mlp_copies(l, f, slot))
            y_acc[...] += mlp_step(h_s[...], w13_s.at[slot], w2_s[slot])

            @pl.when(f + SLOTS < nf)
            def _():
                start(mlp_copies(l, f + SLOTS, slot))
            return 0

        lax.fori_loop(0, nf, mlp, 0)
        x_s[...] = (x_s[...].astype(F32) + y_acc[...]).astype(BF16)
        kc_out.wait()
        vc_out.wait()
        for half in range(2):
            bulk(l, 0, osend_sem.at[l, half], orecv_sem.at[l, half]).wait_send()
        return 0

    lax.fori_loop(0, n_layers, layer, 0)
    out = pltpu.make_async_copy(x_s, y_ref, out_sem.at[0])
    out.start()
    out.wait()


def solution(mesh):
    ncp = mesh.shape['cp']
    act = P(('req', 'cp'), None)
    cache = P(None, 'req', 'cp', None)

    def body(x, pos, g1, g2, wq, wk, wv, wo, w1, w3, w2):
        rows, dim = x.shape
        n_layers, _, ff = w1.shape
        seq = rows * ncp
        tail = ff % FB
        nchip = ncp // CORES
        cos, sin = _angles(pos)
        gains = [g.astype(F32).reshape(n_layers, 1, dim) for g in (g1, g2)]
        vm = pl.BlockSpec(memory_space=pltpu.VMEM)
        hbm = pl.BlockSpec(memory_space=pl.ANY)
        nb = seq // 2 // QB
        y, kc, vc = pl.pallas_call(
            functools.partial(_kernel, ncp),
            out_shape=(jax.ShapeDtypeStruct((rows, dim), BF16),
                       jax.ShapeDtypeStruct((n_layers, seq, HEAD), BF16),
                       jax.ShapeDtypeStruct((n_layers, seq, HEAD), BF16)),
            in_specs=[vm] * 5 + [hbm] * 7,
            out_specs=(hbm,) * 3,
            scratch_shapes=[
                pltpu.VMEM((rows, dim), BF16),
                pltpu.VMEM((rows, dim), BF16),
                pltpu.VMEM((nchip, 3, CORES, rows, HEAD), BF16),
                pltpu.VMEM((n_layers, 3, seq, HEAD), BF16),
                pltpu.VMEM((n_layers, rows, ncp * HEAD), BF16),
                pltpu.VMEM((seq, HEAD), BF16),
                pltpu.VMEM((nb, QB, 128), F32),
                pltpu.VMEM((nb, QB, 128), F32),
                pltpu.VMEM((nb, QB, HEAD), F32),
                pltpu.VMEM((rows, dim), F32),
                pltpu.VMEM((2, 3, dim, CORES * HEAD), BF16),
                pltpu.VMEM((ncp * HEAD, dim), BF16),
                pltpu.VMEM((SLOTS, 2, dim, FB), BF16),
                pltpu.VMEM((SLOTS, FB, dim), BF16),
                pltpu.VMEM((2, dim, tail), BF16),
                pltpu.VMEM((tail, dim), BF16),
                pltpu.SemaphoreType.DMA((n_layers, 2, 3)),
                pltpu.SemaphoreType.DMA((n_layers, 2, 3)),
                pltpu.SemaphoreType.DMA((n_layers, 2)),
                pltpu.SemaphoreType.DMA((n_layers, 2)),
                pltpu.SemaphoreType.DMA((2,)),
                pltpu.SemaphoreType.DMA,
                pltpu.SemaphoreType.DMA((SLOTS,)),
                pltpu.SemaphoreType.DMA,
                pltpu.SemaphoreType.DMA((2,)),
            ],
            compiler_params=pltpu.CompilerParams(collective_id=0, has_side_effects=True,
                                                 vmem_limit_bytes=67043328),
        )(x, cos, sin, *gains, wq, wk, wv, wo, w1, w3, w2)
        return y, kc[:, :, None, :], vc[:, :, None, :]

    return jax.shard_map(body, mesh=mesh, in_specs=(act, P(('req', 'cp'))) + (P(),) * 9,
                         out_specs=(act, cache, cache), check_vma=False)
```

```python
import functools

import jax
import jax.numpy as jnp
from jax import lax
from jax.experimental import pallas as pl
from jax.experimental.pallas import tpu as pltpu
from jax.sharding import PartitionSpec as P

HEAD = 128
F32 = jnp.float32
BF16 = jnp.bfloat16
MESH = pl.DeviceIdType.MESH
CORES = 2
QB = 512
KB = 512
FB = 512
SLOTS = 3
SCALE2 = HEAD ** -0.5 * 1.4426950408889634


def _angles(pos):
    half = HEAD // 2
    inv = 1.0 / (10000.0 ** (jnp.arange(half, dtype=F32) * (2.0 / HEAD)))
    ang = pos.astype(F32)[:, None] * inv
    c, sn = jnp.cos(ang), jnp.sin(ang)
    return jnp.concatenate([c, c], axis=-1), jnp.concatenate([-sn, sn], axis=-1)


def _kernel(ncp, x_ref, cos_ref, sin_ref, g1_ref, g2_ref, wq, wk, wv, wo, w1, w3, w2,
            y_ref, kc_ref, vc_ref,
            x_s, h_s, stage, qkv, o_s, o_stage, m_s, l_s, acc_s, y_acc, relay,
            wqkv_s, wo_s, w13_s, w2_s, w13t_s, w2t_s,
            send_sem, recv_sem, osend_sem, orecv_sem, rrecv_sem, fsend_sem,
            wqkv_sem, wo_sem, wm_sem, wt_sem, out_sem):
    n_layers = wq.shape[0]
    rows, dim = x_ref.shape
    seg = rows // 2
    nseg = 2 * ncp
    seq = nseg * seg
    half_seq = seq // 2
    ff = w1.shape[2]
    nf = ff // FB
    tail = ff - nf * FB
    nchip = ncp // CORES
    last = nchip - 1
    cw = CORES * HEAD
    me = lax.axis_index("cp")
    req = lax.axis_index("req")
    chip, core = me // CORES, me % CORES
    others = (ncp - 1) * seg
    qpasses = [(0, 2)] + [(l, h) for l in range(1, n_layers) for h in range(2)]
    mpasses = [(l, h) for l in range(n_layers - 1) for h in range(2)] + [(n_layers - 1, 2)]
    part = (slice(0, seg), slice(seg, rows), slice(0, rows))

    def chip_at(j):
        off = nchip // 2 + (2 * (j % 2) - 1) * ((j + 1) // 2)
        return lax.rem(chip + off + nchip, nchip)

    def wqkv_copies(p, j):
        slot = (p * nchip + j) % 2 if isinstance(j, int) else lax.rem(p * nchip + j, 2)
        cols = pl.ds(pl.multiple_of(chip_at(j) * cw, cw), cw)
        return [pltpu.make_async_copy(w.at[qpasses[p][0], :, cols], wqkv_s.at[slot, t], wqkv_sem.at[slot])
                for t, w in enumerate((wk, wv, wq))]

    def mlp_copies(p, f, slot):
        l = mpasses[p][0]
        cols = pl.ds(pl.multiple_of(f * FB, FB), FB)
        return [pltpu.make_async_copy(w1.at[l, :, cols], w13_s.at[slot, 0], wm_sem.at[slot]),
                pltpu.make_async_copy(w3.at[l, :, cols], w13_s.at[slot, 1], wm_sem.at[slot]),
                pltpu.make_async_copy(w2.at[l, cols, :], w2_s.at[slot], wm_sem.at[slot])]

    def tail_copies(l):
        cols = pl.ds(nf * FB, tail)
        return [pltpu.make_async_copy(w1.at[l, :, cols], w13t_s.at[0], wt_sem),
                pltpu.make_async_copy(w3.at[l, :, cols], w13t_s.at[1], wt_sem),
                pltpu.make_async_copy(w2.at[l, cols, :], w2t_s, wt_sem)]

    def wo_copies(l):
        return [pltpu.make_async_copy(wo.at[l], wo_s, wo_sem)]

    def start(cs):
        for c in cs:
            c.start()

    def wait(cs):
        for c in cs:
            c.wait()

    def remote(src, dst, ssem, rsem, dev):
        return pltpu.make_async_remote_copy(src_ref=src, dst_ref=dst, send_sem=ssem, recv_sem=rsem,
                                            device_id=(req, dev), device_id_type=MESH)

    def norm(g_ref, l, h):
        blk = 32
        first = part[h].start // blk

        def body(i, _):
            r = pl.ds(pl.multiple_of(i * blk, blk), blk)
            v = x_s[r, :].astype(F32)
            s = lax.rsqrt(jnp.mean(v * v, axis=-1, keepdims=True) + 1e-5)
            h_s[r, :] = (v * s * g_ref[l:l + 1, :].astype(F32)).astype(BF16)
            return 0

        lax.fori_loop(first, part[h].stop // blk, body, 0)

    start(wqkv_copies(0, 0))
    start(wqkv_copies(0, 1))
    barrier = pltpu.get_barrier_semaphore()

    def sig(i, _):
        pl.semaphore_signal(barrier, inc=1, device_id=(req, lax.rem(me + 1 + i, ncp)), device_id_type=MESH)
        return 0

    lax.fori_loop(0, ncp - 1, sig, 0)
    x_s[...] = x_ref[...]

    def row_of(dev, half):
        r = dev * seg if half == 0 else (nseg - 1 - dev) * seg
        return pl.ds(pl.multiple_of(r, seg), seg)

    def piece(l, j, t, hh, half):
        dev = chip_at(j) * CORES + hh
        return remote(stage.at[j, t, hh, pl.ds(half * seg, seg), :], qkv.at[l, t, row_of(me, half), :],
                      send_sem.at[l, half, t], recv_sem.at[l, half, t], dev)

    hop = nchip // 4

    def via(half, sign):
        step = hop if half == 0 else nchip - hop
        return lax.rem(chip + (step if sign > 0 else nchip - step), nchip)

    def send_far(l, half):
        for t in range(3):
            for hh in range(CORES):
                remote(stage.at[0, t, hh, pl.ds(half * seg, seg), :], relay.at[l, half, t, hh],
                       send_sem.at[l, half, t], rrecv_sem.at[l, half], via(half, 1) * CORES + core).start()

    def forward(l, half):
        buf = relay.at[l, half]
        remote(buf, buf, fsend_sem.at[l, half], rrecv_sem.at[l, half], me).wait_recv()
        src = via(half, -1) * CORES + core
        for t in range(3):
            for hh in range(CORES):
                remote(relay.at[l, half, t, hh], qkv.at[l, t, row_of(src, half), :],
                       fsend_sem.at[l, half], recv_sem.at[l, half, t], via(half, 1) * CORES + hh).start()

    def forward_sent(l, half):
        buf = relay.at[l, half]
        remote(buf, buf, fsend_sem.at[l, half], rrecv_sem.at[l, half], me).wait_send()

    def send_chunk(l, j, half, ts=(0, 1, 2)):
        for t in ts:
            for hh in range(CORES):
                piece(l, j, t, hh, half).start()

    def send_sibling(l, half, ts=(0, 1, 2)):
        for t in ts:
            piece(l, last, t, 1 - core, half).start()

    def send_rest(l, half, ts):
        lax.fori_loop(1, last, lambda j, _: (send_chunk(l, j, half, ts), 0)[1], 0)
        send_sibling(l, half, ts)

    def keep_own(l, half):
        for t in range(3):
            qkv[l, t, row_of(me, half), :] = stage[last, t, core, half * seg:(half + 1) * seg, :]

    def project(p):
        l, h = qpasses[p]
        sl = part[h]
        cosv, sinv = cos_ref[sl, :], sin_ref[sl, :]

        def body(j, _):
            slot = lax.rem(p * nchip + j, 2)
            wait(wqkv_copies(p, j))
            a = h_s[sl, :]
            for t in range(3):
                r = jnp.dot(a, wqkv_s[slot, t], preferred_element_type=F32)
                for hh in range(CORES):
                    v = r[:, hh * HEAD:(hh + 1) * HEAD]
                    if t != 1:
                        v = v * cosv + pltpu.roll(v, HEAD // 2, 1) * sinv
                    stage[j, t, hh, sl, :] = v.astype(BF16)

            @pl.when(j + 2 < nchip)
            def _():
                start(wqkv_copies(p, j + 2))

            if p + 1 < len(qpasses):
                @pl.when(j + 2 >= nchip)
                def _():
                    start(wqkv_copies(p + 1, j + 2 - nchip))

            @pl.when(j == 1)
            def _():
                if p == 0:
                    pl.semaphore_wait(barrier, ncp - 1)
                for half in ((0, 1) if h == 2 else (h,)):
                    send_far(l, half)

            @pl.when(j > 1)
            def _():
                send_chunk(l, j - 1, 0 if h == 2 else h)
            return 0

        lax.fori_loop(0, nchip, body, 0)
        send_sibling(l, 0 if h == 2 else h)
        for half in ((0, 1) if h == 2 else (h,)):
            keep_own(l, half)

    def attend(l, qb, kb, st, masked):
        q = qkv[l, 2, pl.ds(pl.multiple_of(qb * QB, QB), QB), :]
        kr = pl.ds(pl.multiple_of(kb * KB, KB), KB)
        s = lax.dot_general(q, qkv[l, 0, kr, :], (((1,), (1,)), ((), ())), preferred_element_type=F32)
        if masked:
            ri = lax.broadcasted_iota(jnp.int32, (QB, KB), 0)
            ci = lax.broadcasted_iota(jnp.int32, (QB, KB), 1)
            s = jnp.where(ci <= ri, s, -jnp.inf)
        m_old = m_s[st]
        m_new = jnp.maximum(m_old, jnp.max(s, axis=1, keepdims=True))
        mc = m_new * SCALE2
        alpha = jnp.exp2(m_old * SCALE2 - mc)
        ps, tot = [], l_s[st] * alpha
        for c in range(KB // 128):
            p = jnp.exp2(s[:, c * 128:(c + 1) * 128] * SCALE2 - mc)
            tot = tot + p
            ps.append(p.astype(BF16))
        m_s[st] = m_new
        l_s[st] = tot
        pv = jnp.dot(jnp.concatenate(ps, axis=1), qkv[l, 1, kr, :], preferred_element_type=F32)
        acc_s[st] = acc_s[st] * alpha + pv

    def attend_init(st):
        m_s[st] = jnp.full((QB, 128), -jnp.inf, F32)
        l_s[st] = jnp.zeros((QB, 128), F32)
        acc_s[st] = jnp.zeros((QB, HEAD), F32)

    my_cols = pl.ds(pl.multiple_of(me * HEAD, HEAD), HEAD)
    nblk = half_seq // QB

    def finish(l, qb, st, half):
        o = (acc_s[st] / jnp.sum(l_s[st], axis=1, keepdims=True)).astype(BF16)
        o_stage[pl.ds(pl.multiple_of(qb * QB, QB), QB), :] = o
        for i in range(QB // seg):
            s_i = qb * (QB // seg) + i
            dev = s_i if half == 0 else nseg - 1 - s_i

            @pl.when(dev == me)
            def _():
                o_s[l, half * seg:(half + 1) * seg, my_cols] = o[i * seg:(i + 1) * seg]

            @pl.when(dev != me)
            def _():
                remote(o_stage.at[pl.ds(pl.multiple_of(s_i * seg, seg), seg), :],
                       o_s.at[l, pl.ds(half * seg, seg), my_cols],
                       osend_sem.at[l, half], orecv_sem.at[l, half], dev).start()

    def attend_a(l):
        def body(qb, _):
            attend_init(qb)
            lax.fori_loop(0, qb, lambda kb, _: (attend(l, qb, kb, qb, False), 0)[1], 0)
            attend(l, qb, qb, qb, True)
            finish(l, qb, qb, 0)
            return 0

        lax.fori_loop(0, nblk, body, 0)

    def attend_ba(l):
        def body(i, _):
            attend_init(i)
            lax.fori_loop(0, nblk, lambda kb, _: (attend(l, nblk + i, kb, i, False), 0)[1], 0)
            return 0

        lax.fori_loop(0, nblk, body, 0)

    def attend_bb(l):
        def body(i, _):
            qb = nblk + i
            lax.fori_loop(nblk, qb, lambda kb, _: (attend(l, qb, kb, i, False), 0)[1], 0)
            attend(l, qb, qb, i, True)
            finish(l, qb, i, 1)
            return 0

        lax.fori_loop(0, nblk, body, 0)

    def bulk(l, t, ssem, rsem):
        r = qkv.at[l, t, pl.ds(0, others), :]
        return remote(r, r, ssem, rsem, me)

    def recv(l, half, ts):
        for t in ts:
            bulk(l, t, send_sem.at[l, half, t], recv_sem.at[l, half, t]).wait_recv()

    def sent(l, half):
        for t in range(3):
            bulk(l, t, send_sem.at[l, half, t], recv_sem.at[l, half, t]).wait_send()
        forward_sent(l, half)

    def o_recv(l, half):
        bulk(l, 0, osend_sem.at[l, half], orecv_sem.at[l, half]).wait_recv()

    def o_sent(l, half):
        bulk(l, 0, osend_sem.at[l, half], orecv_sem.at[l, half]).wait_send()

    def mlp_step(a, w13, w2c):
        g = jnp.dot(a, w13[0], preferred_element_type=F32)
        u = jnp.dot(a, w13[1], preferred_element_type=F32)
        u = (g * (1.0 / (1.0 + jnp.exp(-g))) * u).astype(BF16)
        return jnp.dot(u, w2c, preferred_element_type=F32)

    def dense(p, midway=None):
        l, h = mpasses[p]
        sl = part[h]
        reload = p + 1 < len(mpasses) and mpasses[p + 1][0] != l
        first = p == 0 or mpasses[p - 1][0] != l
        if first:
            wait(wo_copies(l))

        def out_proj(c, _):
            cols = pl.ds(pl.multiple_of(c * FB, FB), FB)
            x_s[sl, cols] = (x_s[sl, cols].astype(F32)
                             + jnp.dot(o_s[l, sl, :], wo_s[:, cols], preferred_element_type=F32)).astype(BF16)
            return 0

        lax.fori_loop(0, dim // FB, out_proj, 0)
        if reload:
            start(wo_copies(l + 1))
        norm(g2_ref, l, h)
        if first:
            wait(tail_copies(l))
        y_acc[sl, :] = mlp_step(h_s[sl, :], w13t_s, w2t_s[...])
        if reload:
            start(tail_copies(l + 1))

        def body(f, _):
            slot = lax.rem(p * nf + f, SLOTS)
            wait(mlp_copies(p, f, slot))
            y_acc[sl, :] += mlp_step(h_s[sl, :], w13_s.at[slot], w2_s[slot])

            @pl.when(f + SLOTS < nf)
            def _():
                start(mlp_copies(p, f + SLOTS, slot))

            if p + 1 < len(mpasses):
                @pl.when(f + SLOTS >= nf)
                def _():
                    start(mlp_copies(p + 1, f + SLOTS - nf, slot))

            if midway is not None:
                pl.when(f == nf // 2)(midway)
            return 0

        lax.fori_loop(0, nf, body, 0)
        x_s[sl, :] = (x_s[sl, :].astype(F32) + y_acc[sl, :]).astype(BF16)

    norm(g1_ref, 0, 2)
    project(0)
    send_rest(0, 1, (2,))
    start(wo_copies(0))
    start(tail_copies(0))
    for f in range(SLOTS):
        start(mlp_copies(0, f, f))
    forward(0, 0)
    forward(0, 1)
    outs = []
    for l in range(n_layers):
        if l > 0:
            o_sent(l - 1, 0)
        recv(l, 0, (0, 1, 2))
        attend_a(l)
        if l == 0:
            send_rest(l, 1, (0, 1))
        else:
            forward(l, 1)
        recv(l, 1, (2,))
        attend_ba(l)
        more = l + 1 < n_layers
        if more:
            o_recv(l, 0)
            dense(2 * l)
            norm(g1_ref, l + 1, 0)
        if l > 0:
            o_sent(l - 1, 1)
        recv(l, 1, (0, 1))
        for i, c in enumerate((kc_ref, vc_ref)):
            cp = pltpu.make_async_copy(qkv.at[l, i], c.at[l], out_sem.at[l, i])
            cp.start()
            outs.append(cp)
        attend_bb(l)
        sent(l, 0)
        if more:
            project(2 * l + 1)
            o_recv(l, 1)
            dense(2 * l + 1, midway=lambda: forward(l + 1, 0))
            norm(g1_ref, l + 1, 1)
            sent(l, 1)
            project(2 * l + 2)
        else:
            sent(l, 1)
            o_recv(l, 0)
            o_recv(l, 1)
            dense(2 * l)
            o_sent(l, 0)
            o_sent(l, 1)
    wait(outs)
    out = pltpu.make_async_copy(x_s, y_ref, out_sem.at[0, 0])
    out.start()
    out.wait()


def _copy_kernel(*refs):
    n = len(refs) // 3
    ins, outs, bufs, rsem, wsem = refs[:n], refs[n:2 * n], refs[2 * n:3 * n], refs[3 * n], refs[3 * n + 1]
    jobs = []
    for a, b, buf in zip(ins, outs, bufs):
        for i in range(a.shape[0]):
            jobs.append((pltpu.make_async_copy(a.at[i], buf.at[i], rsem.at[len(jobs)]),
                         pltpu.make_async_copy(buf.at[i], b.at[i], wsem.at[len(jobs)])))
    for r, _ in jobs:
        r.start()
    for r, w in jobs:
        r.wait()
        w.start()
    for _, w in jobs:
        w.wait()


def _settle(*arrays):
    hbm = pl.BlockSpec(memory_space=pl.ANY)
    n = sum(a.shape[0] for a in arrays)
    return pl.pallas_call(
        _copy_kernel,
        out_shape=tuple(jax.ShapeDtypeStruct(a.shape, a.dtype) for a in arrays),
        in_specs=[hbm] * len(arrays),
        out_specs=(hbm,) * len(arrays),
        scratch_shapes=[pltpu.VMEM(a.shape, a.dtype) for a in arrays]
        + [pltpu.SemaphoreType.DMA((n,)), pltpu.SemaphoreType.DMA((n,))],
    )(*arrays)


def solution(mesh):
    ncp = mesh.shape['cp']
    act = P(('req', 'cp'), None)
    cache = P(None, 'req', 'cp', None)

    def body(x, pos, g1, g2, wq, wk, wv, wo, w1, w3, w2):
        rows, dim = x.shape
        n_layers, _, ff = w1.shape
        seq = rows * ncp
        tail = ff % FB
        nchip = ncp // CORES
        cos, sin = _angles(pos)
        vm = pl.BlockSpec(memory_space=pltpu.VMEM)
        hbm = pl.BlockSpec(memory_space=pl.ANY)
        nb = seq // 2 // QB
        y, kc, vc = pl.pallas_call(
            functools.partial(_kernel, ncp),
            out_shape=(jax.ShapeDtypeStruct((rows, dim), BF16),
                       jax.ShapeDtypeStruct((n_layers, seq, HEAD), BF16),
                       jax.ShapeDtypeStruct((n_layers, seq, HEAD), BF16)),
            in_specs=[vm] * 5 + [hbm] * 7,
            out_specs=(hbm,) * 3,
            scratch_shapes=[
                pltpu.VMEM((rows, dim), BF16),
                pltpu.VMEM((rows, dim), BF16),
                pltpu.VMEM((nchip, 3, CORES, rows, HEAD), BF16),
                pltpu.VMEM((n_layers, 3, seq, HEAD), BF16),
                pltpu.VMEM((n_layers, rows, ncp * HEAD), BF16),
                pltpu.VMEM((seq, HEAD), BF16),
                pltpu.VMEM((nb, QB, 128), F32),
                pltpu.VMEM((nb, QB, 128), F32),
                pltpu.VMEM((nb, QB, HEAD), F32),
                pltpu.VMEM((rows, dim), F32),
                pltpu.VMEM((n_layers, 2, 3, CORES, rows // 2, HEAD), BF16),
                pltpu.VMEM((2, 3, dim, CORES * HEAD), BF16),
                pltpu.VMEM((ncp * HEAD, dim), BF16),
                pltpu.VMEM((SLOTS, 2, dim, FB), BF16),
                pltpu.VMEM((SLOTS, FB, dim), BF16),
                pltpu.VMEM((2, dim, tail), BF16),
                pltpu.VMEM((tail, dim), BF16),
                pltpu.SemaphoreType.DMA((n_layers, 2, 3)),
                pltpu.SemaphoreType.DMA((n_layers, 2, 3)),
                pltpu.SemaphoreType.DMA((n_layers, 2)),
                pltpu.SemaphoreType.DMA((n_layers, 2)),
                pltpu.SemaphoreType.DMA((n_layers, 2)),
                pltpu.SemaphoreType.DMA((n_layers, 2)),
                pltpu.SemaphoreType.DMA((2,)),
                pltpu.SemaphoreType.DMA,
                pltpu.SemaphoreType.DMA((SLOTS,)),
                pltpu.SemaphoreType.DMA,
                pltpu.SemaphoreType.DMA((n_layers, 2)),
            ],
            compiler_params=pltpu.CompilerParams(collective_id=0, has_side_effects=True,
                                                 vmem_limit_bytes=67043328),
        )(x, cos, sin, g1, g2, wq, wk, wv, wo, w1, w3, w2)
        y, kc, vc = _settle(y.reshape(2, rows // 2, dim), kc, vc)
        return y.reshape(rows, dim), kc[:, :, None, :], vc[:, :, None, :]

    return jax.shard_map(body, mesh=mesh, in_specs=(act, P(('req', 'cp'))) + (P(),) * 9,
                         out_specs=(act, cache, cache), check_vma=False)
```

```python
import functools

import jax
import jax.numpy as jnp
from jax import lax
from jax.experimental import pallas as pl
from jax.experimental.pallas import tpu as pltpu
from jax.sharding import PartitionSpec as P

HEAD = 128
F32 = jnp.float32
BF16 = jnp.bfloat16
MESH = pl.DeviceIdType.MESH
CORES = 2
QB = 512
KB = 512
FB = 512
SLOTS = 3
SCALE2 = HEAD ** -0.5 * 1.4426950408889634


def _angles(pos):
    half = HEAD // 2
    inv = 1.0 / (10000.0 ** (jnp.arange(half, dtype=F32) * (2.0 / HEAD)))
    ang = pos.astype(F32)[:, None] * inv
    c, sn = jnp.cos(ang), jnp.sin(ang)
    return jnp.concatenate([c, c], axis=-1), jnp.concatenate([-sn, sn], axis=-1)


def _kernel(ncp, x_ref, cos_ref, sin_ref, g1_ref, g2_ref, wq, wk, wv, wo, w1, w3, w2,
            y_ref, kc_ref, vc_ref,
            x_s, h_s, stage, qkv, o_s, o_stage, m_s, l_s, acc_s, y_acc, relay,
            wqkv_s, wo_s, w13_s, w2_s, w13t_s, w2t_s,
            send_sem, recv_sem, osend_sem, orecv_sem, rsend_sem, rrecv_sem, fsend_sem,
            wqkv_sem, wo_sem, wm_sem, wt_sem, out_sem):
    n_layers = wq.shape[0]
    rows, dim = x_ref.shape
    seg = rows // 2
    nseg = 2 * ncp
    seq = nseg * seg
    half_seq = seq // 2
    ff = w1.shape[2]
    nf = ff // FB
    tail = ff - nf * FB
    nchip = ncp // CORES
    last = nchip - 1
    cw = CORES * HEAD
    me = lax.axis_index("cp")
    req = lax.axis_index("req")
    chip, core = me // CORES, me % CORES
    others = (ncp - 1) * seg
    qpasses = [(0, 2)] + [(l, h) for l in range(1, n_layers) for h in range(2)]
    mpasses = [(l, h) for l in range(n_layers - 1) for h in range(2)] + [(n_layers - 1, 2)]
    part = (slice(0, seg), slice(seg, rows), slice(0, rows))

    def chip_at(j):
        off = nchip // 2 + (2 * (j % 2) - 1) * ((j + 1) // 2)
        return lax.rem(chip + off + nchip, nchip)

    def wqkv_copies(p, j):
        slot = (p * nchip + j) % 2 if isinstance(j, int) else lax.rem(p * nchip + j, 2)
        cols = pl.ds(pl.multiple_of(chip_at(j) * cw, cw), cw)
        return [pltpu.make_async_copy(w.at[qpasses[p][0], :, cols], wqkv_s.at[slot, t], wqkv_sem.at[slot])
                for t, w in enumerate((wk, wv, wq))]

    def mlp_copies(p, f, slot):
        l = mpasses[p][0]
        cols = pl.ds(pl.multiple_of(f * FB, FB), FB)
        return [pltpu.make_async_copy(w1.at[l, :, cols], w13_s.at[slot, 0], wm_sem.at[slot]),
                pltpu.make_async_copy(w3.at[l, :, cols], w13_s.at[slot, 1], wm_sem.at[slot]),
                pltpu.make_async_copy(w2.at[l, cols, :], w2_s.at[slot], wm_sem.at[slot])]

    def tail_copies(l):
        cols = pl.ds(nf * FB, tail)
        return [pltpu.make_async_copy(w1.at[l, :, cols], w13t_s.at[0], wt_sem),
                pltpu.make_async_copy(w3.at[l, :, cols], w13t_s.at[1], wt_sem),
                pltpu.make_async_copy(w2.at[l, cols, :], w2t_s, wt_sem)]

    def wo_copies(l):
        return [pltpu.make_async_copy(wo.at[l], wo_s, wo_sem)]

    def start(cs):
        for c in cs:
            c.start()

    def wait(cs):
        for c in cs:
            c.wait()

    def remote(src, dst, ssem, rsem, dev):
        return pltpu.make_async_remote_copy(src_ref=src, dst_ref=dst, send_sem=ssem, recv_sem=rsem,
                                            device_id=(req, dev), device_id_type=MESH)

    def norm(g_ref, l, h):
        blk = 32
        first = part[h].start // blk

        def body(i, _):
            r = pl.ds(pl.multiple_of(i * blk, blk), blk)
            v = x_s[r, :].astype(F32)
            s = lax.rsqrt(jnp.mean(v * v, axis=-1, keepdims=True) + 1e-5)
            h_s[r, :] = (v * s * g_ref[l:l + 1, :].astype(F32)).astype(BF16)
            return 0

        lax.fori_loop(first, part[h].stop // blk, body, 0)

    start(wqkv_copies(0, 0))
    start(wqkv_copies(0, 1))
    barrier = pltpu.get_barrier_semaphore()

    def sig(i, _):
        pl.semaphore_signal(barrier, inc=1, device_id=(req, lax.rem(me + 1 + i, ncp)), device_id_type=MESH)
        return 0

    lax.fori_loop(0, ncp - 1, sig, 0)
    x_s[...] = x_ref[...]

    def row_of(dev, half):
        r = dev * seg if half == 0 else (nseg - 1 - dev) * seg
        return pl.ds(pl.multiple_of(r, seg), seg)

    A_ALL, B_KV, B_Q = (0, slice(0, 3), 0), (1, slice(0, 2), 1), (1, slice(2, 3), 2)

    def piece(l, j, hh, what):
        half, ts, sem = what
        dev = chip_at(j) * CORES + hh
        return remote(stage.at[j, hh, ts, pl.ds(half * seg, seg), :], qkv.at[l, ts, row_of(me, half), :],
                      send_sem.at[l, sem], recv_sem.at[l, sem], dev)

    def hops(hh, sign):
        step = (nchip // 4) if (hh == 0) == (sign > 0) else nchip - nchip // 4
        return lax.rem(chip + step, nchip)

    def far_copy(l, half, hh):
        return remote(stage.at[0, hh, :, pl.ds(half * seg, seg), :], relay.at[l, half, hh],
                      rsend_sem.at[l, half, hh], rrecv_sem.at[l, half, hh], hops(hh, 1) * CORES + core)

    def send_far(l, half):
        for hh in range(CORES):
            far_copy(l, half, hh).start()

    def forward_copies(l, half, hh):
        src = hops(hh, -1) * CORES + core
        return [remote(relay.at[l, half, hh, ts], qkv.at[l, ts, row_of(src, half), :],
                       fsend_sem.at[l, half, hh, i], recv_sem.at[l, sem], hops(hh, 1) * CORES + hh)
                for i, (_, ts, sem) in enumerate((A_ALL,) if half == 0 else (B_Q, B_KV))]

    def forward(l, half):
        for hh in range(CORES):
            far_copy(l, half, hh).wait_recv()
            start(forward_copies(l, half, hh))

    def send_chunk(l, j, what):
        for hh in range(CORES):
            piece(l, j, hh, what).start()

    def send_sibling(l, what):
        piece(l, last, 1 - core, what).start()

    def send_rest(l, what):
        lax.fori_loop(1, last, lambda j, _: (send_chunk(l, j, what), 0)[1], 0)
        send_sibling(l, what)

    def keep_own(l, half):
        qkv[l, :, row_of(me, half), :] = stage[last, core, :, half * seg:(half + 1) * seg, :]

    def project(p):
        l, h = qpasses[p]
        sl = part[h]
        cosv, sinv = cos_ref[sl, :], sin_ref[sl, :]

        def body(j, _):
            slot = lax.rem(p * nchip + j, 2)
            wait(wqkv_copies(p, j))
            a = h_s[sl, :]
            for t in range(3):
                r = jnp.dot(a, wqkv_s[slot, t], preferred_element_type=F32)
                for hh in range(CORES):
                    v = r[:, hh * HEAD:(hh + 1) * HEAD]
                    if t != 1:
                        v = v * cosv + pltpu.roll(v, HEAD // 2, 1) * sinv
                    stage[j, hh, t, sl, :] = v.astype(BF16)

            @pl.when(j + 2 < nchip)
            def _():
                start(wqkv_copies(p, j + 2))

            if p + 1 < len(qpasses):
                @pl.when(j + 2 >= nchip)
                def _():
                    start(wqkv_copies(p + 1, j + 2 - nchip))

            @pl.when(j == 1)
            def _():
                if p == 0:
                    pl.semaphore_wait(barrier, ncp - 1)
                send_far(l, 0 if h == 2 else h)

            @pl.when(j > 1)
            def _():
                for what in ((B_Q, B_KV) if h == 1 else (A_ALL,)):
                    send_chunk(l, j - 1, what)
            return 0

        lax.fori_loop(0, nchip, body, 0)
        for what in ((B_Q, B_KV) if h == 1 else (A_ALL,)):
            send_sibling(l, what)
        for half in ((0, 1) if h == 2 else (h,)):
            keep_own(l, half)

    def attend(l, qb, kb, st, masked):
        q = qkv[l, 2, pl.ds(pl.multiple_of(qb * QB, QB), QB), :]
        kr = pl.ds(pl.multiple_of(kb * KB, KB), KB)
        s = lax.dot_general(q, qkv[l, 0, kr, :], (((1,), (1,)), ((), ())), preferred_element_type=F32)
        if masked:
            ri = lax.broadcasted_iota(jnp.int32, (QB, KB), 0)
            ci = lax.broadcasted_iota(jnp.int32, (QB, KB), 1)
            s = jnp.where(ci <= ri, s, -jnp.inf)
        m_old = m_s[st]
        m_new = jnp.maximum(m_old, jnp.max(s, axis=1, keepdims=True))
        mc = m_new * SCALE2
        alpha = jnp.exp2(m_old * SCALE2 - mc)
        ps, tot = [], l_s[st] * alpha
        for c in range(KB // 128):
            p = jnp.exp2(s[:, c * 128:(c + 1) * 128] * SCALE2 - mc)
            tot = tot + p
            ps.append(p.astype(BF16))
        m_s[st] = m_new
        l_s[st] = tot
        pv = jnp.dot(jnp.concatenate(ps, axis=1), qkv[l, 1, kr, :], preferred_element_type=F32)
        acc_s[st] = acc_s[st] * alpha + pv

    def attend_init(st):
        m_s[st] = jnp.full((QB, 128), -jnp.inf, F32)
        l_s[st] = jnp.zeros((QB, 128), F32)
        acc_s[st] = jnp.zeros((QB, HEAD), F32)

    my_cols = pl.ds(pl.multiple_of(me * HEAD, HEAD), HEAD)
    nblk = half_seq // QB

    def finish(l, qb, st, half):
        o = (acc_s[st] / jnp.sum(l_s[st], axis=1, keepdims=True)).astype(BF16)
        o_stage[pl.ds(pl.multiple_of(qb * QB, QB), QB), :] = o
        for i in range(QB // seg):
            s_i = qb * (QB // seg) + i
            dev = s_i if half == 0 else nseg - 1 - s_i

            @pl.when(dev == me)
            def _():
                o_s[l, half * seg:(half + 1) * seg, my_cols] = o[i * seg:(i + 1) * seg]

            @pl.when(dev != me)
            def _():
                remote(o_stage.at[pl.ds(pl.multiple_of(s_i * seg, seg), seg), :],
                       o_s.at[l, pl.ds(half * seg, seg), my_cols],
                       osend_sem.at[l, half], orecv_sem.at[l, half], dev).start()

    def attend_a(l):
        def body(qb, _):
            attend_init(qb)
            lax.fori_loop(0, qb, lambda kb, _: (attend(l, qb, kb, qb, False), 0)[1], 0)
            attend(l, qb, qb, qb, True)
            finish(l, qb, qb, 0)
            return 0

        lax.fori_loop(0, nblk, body, 0)

    def attend_ba(l):
        def body(i, _):
            attend_init(i)
            lax.fori_loop(0, nblk, lambda kb, _: (attend(l, nblk + i, kb, i, False), 0)[1], 0)
            return 0

        lax.fori_loop(0, nblk, body, 0)

    def attend_bb(l):
        def body(i, _):
            qb = nblk + i
            lax.fori_loop(nblk, qb, lambda kb, _: (attend(l, qb, kb, i, False), 0)[1], 0)
            attend(l, qb, qb, i, True)
            finish(l, qb, i, 1)
            return 0

        lax.fori_loop(0, nblk, body, 0)

    def bulk(l, ts, n, ssem, rsem):
        r = qkv.at[l, ts, pl.ds(0, n * seg), :]
        return remote(r, r, ssem, rsem, me)

    def recv(l, what):
        bulk(l, what[1], ncp - 1, send_sem.at[l, what[2]], recv_sem.at[l, what[2]]).wait_recv()

    def sent(l, half):
        for _, ts, sem in ((A_ALL,) if half == 0 else (B_Q, B_KV)):
            bulk(l, ts, ncp - 1 - CORES, send_sem.at[l, sem], recv_sem.at[l, sem]).wait_send()
        for hh in range(CORES):
            far_copy(l, half, hh).wait_send()
            for c in forward_copies(l, half, hh):
                c.wait_send()

    def o_recv(l, half):
        bulk(l, slice(0, 1), ncp - 1, osend_sem.at[l, half], orecv_sem.at[l, half]).wait_recv()

    def o_sent(l, half):
        bulk(l, slice(0, 1), ncp - 1, osend_sem.at[l, half], orecv_sem.at[l, half]).wait_send()

    def mlp_step(a, w13, w2c):
        g = jnp.dot(a, w13[0], preferred_element_type=F32)
        u = jnp.dot(a, w13[1], preferred_element_type=F32)
        u = (g * (1.0 / (1.0 + jnp.exp(-g))) * u).astype(BF16)
        return jnp.dot(u, w2c, preferred_element_type=F32)

    def dense(p, midway=None):
        l, h = mpasses[p]
        sl = part[h]
        reload = p + 1 < len(mpasses) and mpasses[p + 1][0] != l
        first = p == 0 or mpasses[p - 1][0] != l
        if first:
            wait(wo_copies(l))

        def out_proj(c, _):
            cols = pl.ds(pl.multiple_of(c * FB, FB), FB)
            x_s[sl, cols] = (x_s[sl, cols].astype(F32)
                             + jnp.dot(o_s[l, sl, :], wo_s[:, cols], preferred_element_type=F32)).astype(BF16)
            return 0

        lax.fori_loop(0, dim // FB, out_proj, 0)
        if reload:
            start(wo_copies(l + 1))
        norm(g2_ref, l, h)
        if first:
            wait(tail_copies(l))
        y_acc[sl, :] = mlp_step(h_s[sl, :], w13t_s, w2t_s[...])
        if reload:
            start(tail_copies(l + 1))

        def body(f, _):
            slot = lax.rem(p * nf + f, SLOTS)
            wait(mlp_copies(p, f, slot))
            y_acc[sl, :] += mlp_step(h_s[sl, :], w13_s.at[slot], w2_s[slot])

            @pl.when(f + SLOTS < nf)
            def _():
                start(mlp_copies(p, f + SLOTS, slot))

            if p + 1 < len(mpasses):
                @pl.when(f + SLOTS >= nf)
                def _():
                    start(mlp_copies(p + 1, f + SLOTS - nf, slot))

            if midway is not None:
                pl.when(f == nf // 2)(midway)
            return 0

        lax.fori_loop(0, nf, body, 0)
        x_s[sl, :] = (x_s[sl, :].astype(F32) + y_acc[sl, :]).astype(BF16)

    norm(g1_ref, 0, 2)
    project(0)
    send_far(0, 1)
    send_rest(0, B_Q)
    start(wo_copies(0))
    start(tail_copies(0))
    for f in range(SLOTS):
        start(mlp_copies(0, f, f))
    forward(0, 0)
    outs = []
    for l in range(n_layers):
        if l > 0:
            o_sent(l - 1, 0)
        recv(l, A_ALL)
        attend_a(l)
        if l == 0:
            send_rest(l, B_KV)
        forward(l, 1)
        recv(l, B_Q)
        attend_ba(l)
        more = l + 1 < n_layers
        if more:
            o_recv(l, 0)
            dense(2 * l)
            norm(g1_ref, l + 1, 0)
        if l > 0:
            o_sent(l - 1, 1)
        recv(l, B_KV)
        for i, c in enumerate((kc_ref, vc_ref)):
            cp = pltpu.make_async_copy(qkv.at[l, i], c.at[l], out_sem.at[l, i])
            cp.start()
            outs.append(cp)
        attend_bb(l)
        sent(l, 0)
        if more:
            project(2 * l + 1)
            o_recv(l, 1)
            dense(2 * l + 1, midway=lambda: forward(l + 1, 0))
            norm(g1_ref, l + 1, 1)
            sent(l, 1)
            project(2 * l + 2)
        else:
            sent(l, 1)
            o_recv(l, 0)
            o_recv(l, 1)
            dense(2 * l)
            o_sent(l, 0)
            o_sent(l, 1)
    wait(outs)
    out = pltpu.make_async_copy(x_s, y_ref, out_sem.at[0, 0])
    out.start()
    out.wait()


def _copy_kernel(*refs):
    n = len(refs) // 3
    ins, outs, bufs, rsem, wsem = refs[:n], refs[n:2 * n], refs[2 * n:3 * n], refs[3 * n], refs[3 * n + 1]
    jobs = []
    for a, b, buf in zip(ins, outs, bufs):
        for i in range(a.shape[0]):
            jobs.append((pltpu.make_async_copy(a.at[i], buf.at[i], rsem.at[len(jobs)]),
                         pltpu.make_async_copy(buf.at[i], b.at[i], wsem.at[len(jobs)])))
    for r, _ in jobs:
        r.start()
    for r, w in jobs:
        r.wait()
        w.start()
    for _, w in jobs:
        w.wait()


def _settle(*arrays):
    hbm = pl.BlockSpec(memory_space=pl.ANY)
    n = sum(a.shape[0] for a in arrays)
    return pl.pallas_call(
        _copy_kernel,
        out_shape=tuple(jax.ShapeDtypeStruct(a.shape, a.dtype) for a in arrays),
        in_specs=[hbm] * len(arrays),
        out_specs=(hbm,) * len(arrays),
        scratch_shapes=[pltpu.VMEM(a.shape, a.dtype) for a in arrays]
        + [pltpu.SemaphoreType.DMA((n,)), pltpu.SemaphoreType.DMA((n,))],
    )(*arrays)


def solution(mesh):
    ncp = mesh.shape['cp']
    act = P(('req', 'cp'), None)
    cache = P(None, 'req', 'cp', None)

    def body(x, pos, g1, g2, wq, wk, wv, wo, w1, w3, w2):
        rows, dim = x.shape
        n_layers, _, ff = w1.shape
        seq = rows * ncp
        tail = ff % FB
        nchip = ncp // CORES
        cos, sin = _angles(pos)
        vm = pl.BlockSpec(memory_space=pltpu.VMEM)
        hbm = pl.BlockSpec(memory_space=pl.ANY)
        nb = seq // 2 // QB
        y, kc, vc = pl.pallas_call(
            functools.partial(_kernel, ncp),
            out_shape=(jax.ShapeDtypeStruct((rows, dim), BF16),
                       jax.ShapeDtypeStruct((n_layers, seq, HEAD), BF16),
                       jax.ShapeDtypeStruct((n_layers, seq, HEAD), BF16)),
            in_specs=[vm] * 5 + [hbm] * 7,
            out_specs=(hbm,) * 3,
            scratch_shapes=[
                pltpu.VMEM((rows, dim), BF16),
                pltpu.VMEM((rows, dim), BF16),
                pltpu.VMEM((nchip, CORES, 3, rows, HEAD), BF16),
                pltpu.VMEM((n_layers, 3, seq, HEAD), BF16),
                pltpu.VMEM((n_layers, rows, ncp * HEAD), BF16),
                pltpu.VMEM((seq, HEAD), BF16),
                pltpu.VMEM((nb, QB, 128), F32),
                pltpu.VMEM((nb, QB, 128), F32),
                pltpu.VMEM((nb, QB, HEAD), F32),
                pltpu.VMEM((rows, dim), F32),
                pltpu.VMEM((n_layers, 2, CORES, 3, rows // 2, HEAD), BF16),
                pltpu.VMEM((2, 3, dim, CORES * HEAD), BF16),
                pltpu.VMEM((ncp * HEAD, dim), BF16),
                pltpu.VMEM((SLOTS, 2, dim, FB), BF16),
                pltpu.VMEM((SLOTS, FB, dim), BF16),
                pltpu.VMEM((2, dim, tail), BF16),
                pltpu.VMEM((tail, dim), BF16),
                pltpu.SemaphoreType.DMA((n_layers, 3)),
                pltpu.SemaphoreType.DMA((n_layers, 3)),
                pltpu.SemaphoreType.DMA((n_layers, 2)),
                pltpu.SemaphoreType.DMA((n_layers, 2)),
                pltpu.SemaphoreType.DMA((n_layers, 2, CORES)),
                pltpu.SemaphoreType.DMA((n_layers, 2, CORES)),
                pltpu.SemaphoreType.DMA((n_layers, 2, CORES, 2)),
                pltpu.SemaphoreType.DMA((2,)),
                pltpu.SemaphoreType.DMA,
                pltpu.SemaphoreType.DMA((SLOTS,)),
                pltpu.SemaphoreType.DMA,
                pltpu.SemaphoreType.DMA((n_layers, 2)),
            ],
            compiler_params=pltpu.CompilerParams(collective_id=0, has_side_effects=True,
                                                 vmem_limit_bytes=67043328),
        )(x, cos, sin, g1, g2, wq, wk, wv, wo, w1, w3, w2)
        y, kc, vc = _settle(y.reshape(2, rows // 2, dim), kc, vc)
        return y.reshape(rows, dim), kc[:, :, None, :], vc[:, :, None, :]

    return jax.shard_map(body, mesh=mesh, in_specs=(act, P(('req', 'cp'))) + (P(),) * 9,
                         out_specs=(act, cache, cache), check_vma=False)
```

```python
import functools

import jax
import jax.numpy as jnp
from jax import lax
from jax.experimental import pallas as pl
from jax.experimental.pallas import tpu as pltpu
from jax.sharding import PartitionSpec as P

HEAD = 128
F32 = jnp.float32
BF16 = jnp.bfloat16
MESH = pl.DeviceIdType.MESH
CORES = 2
QB = 512
KB = 512
FB = 512
SLOTS = 3
SCALE2 = HEAD ** -0.5 * 1.4426950408889634


def _angles(pos):
    half = HEAD // 2
    inv = 1.0 / (10000.0 ** (jnp.arange(half, dtype=F32) * (2.0 / HEAD)))
    ang = pos.astype(F32)[:, None] * inv
    c, sn = jnp.cos(ang), jnp.sin(ang)
    return jnp.concatenate([c, c], axis=-1), jnp.concatenate([-sn, sn], axis=-1)


def _kernel(ncp, x_ref, cos_ref, sin_ref, g1_ref, g2_ref, wq, wk, wv, wo, w1, w3, w2,
            y_ref, kc_ref, vc_ref,
            x_s, h_s, stage, qkv, o_s, o_stage, m_s, l_s, acc_s, y_acc,
            wqkv_s, wo_s, w13_s, w2_s, w13t_s, w2t_s,
            send_sem, recv_sem, osend_sem, orecv_sem,
            wqkv_sem, wo_sem, wm_sem, wt_sem, out_sem):
    n_layers = wq.shape[0]
    rows, dim = x_ref.shape
    seg = rows // 2
    nseg = 2 * ncp
    seq = nseg * seg
    half_seq = seq // 2
    ff = w1.shape[2]
    nf = ff // FB
    tail = ff - nf * FB
    nchip = ncp // CORES
    last = nchip - 1
    cw = CORES * HEAD
    me = lax.axis_index("cp")
    req = lax.axis_index("req")
    chip, core = me // CORES, me % CORES
    others = (ncp - 1) * seg
    qpasses = [(0, 2)] + [(l, h) for l in range(1, n_layers) for h in range(2)]
    mpasses = [(l, h) for l in range(n_layers - 1) for h in range(2)] + [(n_layers - 1, 2)]
    part = (slice(0, seg), slice(seg, rows), slice(0, rows))

    def chip_at(j):
        off = nchip // 2 + (2 * (j % 2) - 1) * ((j + 1) // 2)
        return lax.rem(chip + off + nchip, nchip)

    def wqkv_copies(p, j):
        slot = (p * nchip + j) % 2 if isinstance(j, int) else lax.rem(p * nchip + j, 2)
        cols = pl.ds(pl.multiple_of(chip_at(j) * cw, cw), cw)
        return [pltpu.make_async_copy(w.at[qpasses[p][0], :, cols], wqkv_s.at[slot, t], wqkv_sem.at[slot])
                for t, w in enumerate((wk, wv, wq))]

    def mlp_copies(p, f, slot):
        l = mpasses[p][0]
        cols = pl.ds(pl.multiple_of(f * FB, FB), FB)
        return [pltpu.make_async_copy(w1.at[l, :, cols], w13_s.at[slot, 0], wm_sem.at[slot]),
                pltpu.make_async_copy(w3.at[l, :, cols], w13_s.at[slot, 1], wm_sem.at[slot]),
                pltpu.make_async_copy(w2.at[l, cols, :], w2_s.at[slot], wm_sem.at[slot])]

    def tail_copies(l):
        cols = pl.ds(nf * FB, tail)
        return [pltpu.make_async_copy(w1.at[l, :, cols], w13t_s.at[0], wt_sem),
                pltpu.make_async_copy(w3.at[l, :, cols], w13t_s.at[1], wt_sem),
                pltpu.make_async_copy(w2.at[l, cols, :], w2t_s, wt_sem)]

    def wo_copies(l):
        return [pltpu.make_async_copy(wo.at[l], wo_s, wo_sem)]

    def start(cs):
        for c in cs:
            c.start()

    def wait(cs):
        for c in cs:
            c.wait()

    def remote(src, dst, ssem, rsem, dev):
        return pltpu.make_async_remote_copy(src_ref=src, dst_ref=dst, send_sem=ssem, recv_sem=rsem,
                                            device_id=(req, dev), device_id_type=MESH)

    def norm(g_ref, l, h):
        blk = 32
        first = part[h].start // blk

        def body(i, _):
            r = pl.ds(pl.multiple_of(i * blk, blk), blk)
            v = x_s[r, :].astype(F32)
            s = lax.rsqrt(jnp.mean(v * v, axis=-1, keepdims=True) + 1e-5)
            h_s[r, :] = (v * s * g_ref[l:l + 1, :].astype(F32)).astype(BF16)
            return 0

        lax.fori_loop(first, part[h].stop // blk, body, 0)

    start(wqkv_copies(0, 0))
    start(wqkv_copies(0, 1))
    barrier = pltpu.get_barrier_semaphore()

    def sig(i, _):
        pl.semaphore_signal(barrier, inc=1, device_id=(req, lax.rem(me + 1 + i, ncp)), device_id_type=MESH)
        return 0

    lax.fori_loop(0, ncp - 1, sig, 0)
    x_s[...] = x_ref[...]

    def row_of(dev, half):
        r = dev * seg if half == 0 else (nseg - 1 - dev) * seg
        return pl.ds(pl.multiple_of(r, seg), seg)

    A_ALL, B_KV, B_Q = (0, slice(0, 3), 0), (1, slice(0, 2), 1), (1, slice(2, 3), 2)

    def piece(l, j, hh, what):
        half, ts, sem = what
        dev = chip_at(j) * CORES + hh
        return remote(stage.at[j, hh, ts, pl.ds(half * seg, seg), :], qkv.at[l, ts, row_of(me, half), :],
                      send_sem.at[l, sem], recv_sem.at[l, sem], dev)

    def send_chunk(l, j, what):
        for hh in range(CORES):
            piece(l, j, hh, what).start()

    def send_sibling(l, what):
        piece(l, last, 1 - core, what).start()

    def send_all(l, what):
        lax.fori_loop(0, last, lambda j, _: (send_chunk(l, j, what), 0)[1], 0)
        send_sibling(l, what)

    def keep_own(l, half):
        qkv[l, :, row_of(me, half), :] = stage[last, core, :, half * seg:(half + 1) * seg, :]

    def project(p):
        l, h = qpasses[p]
        sl = part[h]
        cosv, sinv = cos_ref[sl, :], sin_ref[sl, :]

        def body(j, _):
            slot = lax.rem(p * nchip + j, 2)
            wait(wqkv_copies(p, j))
            a = h_s[sl, :]
            for t in range(3):
                r = jnp.dot(a, wqkv_s[slot, t], preferred_element_type=F32)
                for hh in range(CORES):
                    v = r[:, hh * HEAD:(hh + 1) * HEAD]
                    if t != 1:
                        v = v * cosv + pltpu.roll(v, HEAD // 2, 1) * sinv
                    stage[j, hh, t, sl, :] = v.astype(BF16)

            @pl.when(j + 2 < nchip)
            def _():
                start(wqkv_copies(p, j + 2))

            if p + 1 < len(qpasses):
                @pl.when(j + 2 >= nchip)
                def _():
                    start(wqkv_copies(p + 1, j + 2 - nchip))

            if p == 0:
                @pl.when(j == 1)
                def _():
                    pl.semaphore_wait(barrier, ncp - 1)

            @pl.when(j > 0)
            def _():
                send_chunk(l, j - 1, B_Q if h == 1 else A_ALL)
            return 0

        lax.fori_loop(0, nchip, body, 0)
        send_sibling(l, B_Q if h == 1 else A_ALL)
        if h == 1:
            send_all(l, B_KV)
        for half in ((0, 1) if h == 2 else (h,)):
            keep_own(l, half)

    def attend(l, qb, kb, st, masked):
        q = qkv[l, 2, pl.ds(pl.multiple_of(qb * QB, QB), QB), :]
        kr = pl.ds(pl.multiple_of(kb * KB, KB), KB)
        s = lax.dot_general(q, qkv[l, 0, kr, :], (((1,), (1,)), ((), ())), preferred_element_type=F32)
        if masked:
            ri = lax.broadcasted_iota(jnp.int32, (QB, KB), 0)
            ci = lax.broadcasted_iota(jnp.int32, (QB, KB), 1)
            s = jnp.where(ci <= ri, s, -jnp.inf)
        m_old = m_s[st]
        m_new = jnp.maximum(m_old, jnp.max(s, axis=1, keepdims=True))
        mc = m_new * SCALE2
        alpha = jnp.exp2(m_old * SCALE2 - mc)
        ps, tot = [], l_s[st] * alpha
        for c in range(KB // 128):
            p = jnp.exp2(s[:, c * 128:(c + 1) * 128] * SCALE2 - mc)
            tot = tot + p
            ps.append(p.astype(BF16))
        m_s[st] = m_new
        l_s[st] = tot
        pv = jnp.dot(jnp.concatenate(ps, axis=1), qkv[l, 1, kr, :], preferred_element_type=F32)
        acc_s[st] = acc_s[st] * alpha + pv

    def attend_init(st):
        m_s[st] = jnp.full((QB, 128), -jnp.inf, F32)
        l_s[st] = jnp.zeros((QB, 128), F32)
        acc_s[st] = jnp.zeros((QB, HEAD), F32)

    my_cols = pl.ds(pl.multiple_of(me * HEAD, HEAD), HEAD)
    nblk = half_seq // QB

    def finish(l, qb, st, half):
        o = (acc_s[st] / jnp.sum(l_s[st], axis=1, keepdims=True)).astype(BF16)
        o_stage[pl.ds(pl.multiple_of(qb * QB, QB), QB), :] = o
        for i in range(QB // seg):
            s_i = qb * (QB // seg) + i
            dev = s_i if half == 0 else nseg - 1 - s_i

            @pl.when(dev == me)
            def _():
                o_s[l, half * seg:(half + 1) * seg, my_cols] = o[i * seg:(i + 1) * seg]

            @pl.when(dev != me)
            def _():
                remote(o_stage.at[pl.ds(pl.multiple_of(s_i * seg, seg), seg), :],
                       o_s.at[l, pl.ds(half * seg, seg), my_cols],
                       osend_sem.at[l, half], orecv_sem.at[l, half], dev).start()

    def attend_a(l):
        def body(qb, _):
            attend_init(qb)
            lax.fori_loop(0, qb, lambda kb, _: (attend(l, qb, kb, qb, False), 0)[1], 0)
            attend(l, qb, qb, qb, True)
            finish(l, qb, qb, 0)
            return 0

        lax.fori_loop(0, nblk, body, 0)

    def attend_ba(l):
        def body(i, _):
            attend_init(i)
            lax.fori_loop(0, nblk, lambda kb, _: (attend(l, nblk + i, kb, i, False), 0)[1], 0)
            return 0

        lax.fori_loop(0, nblk, body, 0)

    def attend_bb(l):
        def body(i, _):
            qb = nblk + i
            lax.fori_loop(nblk, qb, lambda kb, _: (attend(l, qb, kb, i, False), 0)[1], 0)
            attend(l, qb, qb, i, True)
            finish(l, qb, i, 1)
            return 0

        lax.fori_loop(0, nblk, body, 0)

    def bulk(l, ts, n, ssem, rsem):
        r = qkv.at[l, ts, pl.ds(0, n * seg), :]
        return remote(r, r, ssem, rsem, me)

    def recv(l, what):
        bulk(l, what[1], ncp - 1, send_sem.at[l, what[2]], recv_sem.at[l, what[2]]).wait_recv()

    def sent(l, half):
        for _, ts, sem in ((A_ALL,) if half == 0 else (B_Q, B_KV)):
            bulk(l, ts, ncp - 1, send_sem.at[l, sem], recv_sem.at[l, sem]).wait_send()

    def o_recv(l, half):
        bulk(l, slice(0, 1), ncp - 1, osend_sem.at[l, half], orecv_sem.at[l, half]).wait_recv()

    def o_sent(l, half):
        bulk(l, slice(0, 1), ncp - 1, osend_sem.at[l, half], orecv_sem.at[l, half]).wait_send()

    def mlp_step(a, w13, w2c):
        g = jnp.dot(a, w13[0], preferred_element_type=F32)
        u = jnp.dot(a, w13[1], preferred_element_type=F32)
        u = (g * (1.0 / (1.0 + jnp.exp(-g))) * u).astype(BF16)
        return jnp.dot(u, w2c, preferred_element_type=F32)

    def dense(p):
        l, h = mpasses[p]
        sl = part[h]
        reload = p + 1 < len(mpasses) and mpasses[p + 1][0] != l
        first = p == 0 or mpasses[p - 1][0] != l
        if first:
            wait(wo_copies(l))

        def out_proj(c, _):
            cols = pl.ds(pl.multiple_of(c * FB, FB), FB)
            x_s[sl, cols] = (x_s[sl, cols].astype(F32)
                             + jnp.dot(o_s[l, sl, :], wo_s[:, cols], preferred_element_type=F32)).astype(BF16)
            return 0

        lax.fori_loop(0, dim // FB, out_proj, 0)
        if reload:
            start(wo_copies(l + 1))
        norm(g2_ref, l, h)
        if first:
            wait(tail_copies(l))
        y_acc[sl, :] = mlp_step(h_s[sl, :], w13t_s, w2t_s[...])
        if reload:
            start(tail_copies(l + 1))

        def body(f, _):
            slot = lax.rem(p * nf + f, SLOTS)
            wait(mlp_copies(p, f, slot))
            y_acc[sl, :] += mlp_step(h_s[sl, :], w13_s.at[slot], w2_s[slot])

            @pl.when(f + SLOTS < nf)
            def _():
                start(mlp_copies(p, f + SLOTS, slot))

            if p + 1 < len(mpasses):
                @pl.when(f + SLOTS >= nf)
                def _():
                    start(mlp_copies(p + 1, f + SLOTS - nf, slot))

            return 0

        lax.fori_loop(0, nf, body, 0)
        x_s[sl, :] = (x_s[sl, :].astype(F32) + y_acc[sl, :]).astype(BF16)

    norm(g1_ref, 0, 2)
    project(0)
    send_all(0, B_Q)
    start(wo_copies(0))
    start(tail_copies(0))
    for f in range(SLOTS):
        start(mlp_copies(0, f, f))
    outs = []
    for l in range(n_layers):
        if l > 0:
            o_sent(l - 1, 0)
        recv(l, A_ALL)
        attend_a(l)
        if l == 0:
            send_all(l, B_KV)
        recv(l, B_Q)
        attend_ba(l)
        more = l + 1 < n_layers
        if more:
            o_recv(l, 0)
            dense(2 * l)
            norm(g1_ref, l + 1, 0)
        if l > 0:
            o_sent(l - 1, 1)
        recv(l, B_KV)
        for i, c in enumerate((kc_ref, vc_ref)):
            cp = pltpu.make_async_copy(qkv.at[l, i], c.at[l], out_sem.at[l, i])
            cp.start()
            outs.append(cp)
        attend_bb(l)
        sent(l, 0)
        if more:
            project(2 * l + 1)
            o_recv(l, 1)
            dense(2 * l + 1)
            norm(g1_ref, l + 1, 1)
            sent(l, 1)
            project(2 * l + 2)
        else:
            sent(l, 1)
            o_recv(l, 0)
            o_recv(l, 1)
            dense(2 * l)
            o_sent(l, 0)
            o_sent(l, 1)
    wait(outs)
    out = pltpu.make_async_copy(x_s, y_ref, out_sem.at[0, 0])
    out.start()
    out.wait()


def _copy_kernel(*refs):
    n = len(refs) // 3
    ins, outs, bufs, rsem, wsem = refs[:n], refs[n:2 * n], refs[2 * n:3 * n], refs[3 * n], refs[3 * n + 1]
    jobs = []
    for a, b, buf in zip(ins, outs, bufs):
        for i in range(a.shape[0]):
            jobs.append((pltpu.make_async_copy(a.at[i], buf.at[i], rsem.at[len(jobs)]),
                         pltpu.make_async_copy(buf.at[i], b.at[i], wsem.at[len(jobs)])))
    for r, _ in jobs:
        r.start()
    for r, w in jobs:
        r.wait()
        w.start()
    for _, w in jobs:
        w.wait()


def _settle(*arrays):
    hbm = pl.BlockSpec(memory_space=pl.ANY)
    n = sum(a.shape[0] for a in arrays)
    return pl.pallas_call(
        _copy_kernel,
        out_shape=tuple(jax.ShapeDtypeStruct(a.shape, a.dtype) for a in arrays),
        in_specs=[hbm] * len(arrays),
        out_specs=(hbm,) * len(arrays),
        scratch_shapes=[pltpu.VMEM(a.shape, a.dtype) for a in arrays]
        + [pltpu.SemaphoreType.DMA((n,)), pltpu.SemaphoreType.DMA((n,))],
    )(*arrays)


def solution(mesh):
    ncp = mesh.shape['cp']
    act = P(('req', 'cp'), None)
    cache = P(None, 'req', 'cp', None)

    def body(x, pos, g1, g2, wq, wk, wv, wo, w1, w3, w2):
        rows, dim = x.shape
        n_layers, _, ff = w1.shape
        seq = rows * ncp
        tail = ff % FB
        nchip = ncp // CORES
        cos, sin = _angles(pos)
        vm = pl.BlockSpec(memory_space=pltpu.VMEM)
        hbm = pl.BlockSpec(memory_space=pl.ANY)
        nb = seq // 2 // QB
        y, kc, vc = pl.pallas_call(
            functools.partial(_kernel, ncp),
            out_shape=(jax.ShapeDtypeStruct((rows, dim), BF16),
                       jax.ShapeDtypeStruct((n_layers, seq, HEAD), BF16),
                       jax.ShapeDtypeStruct((n_layers, seq, HEAD), BF16)),
            in_specs=[vm] * 5 + [hbm] * 7,
            out_specs=(hbm,) * 3,
            scratch_shapes=[
                pltpu.VMEM((rows, dim), BF16),
                pltpu.VMEM((rows, dim), BF16),
                pltpu.VMEM((nchip, CORES, 3, rows, HEAD), BF16),
                pltpu.VMEM((n_layers, 3, seq, HEAD), BF16),
                pltpu.VMEM((n_layers, rows, ncp * HEAD), BF16),
                pltpu.VMEM((seq, HEAD), BF16),
                pltpu.VMEM((nb, QB, 128), F32),
                pltpu.VMEM((nb, QB, 128), F32),
                pltpu.VMEM((nb, QB, HEAD), F32),
                pltpu.VMEM((rows, dim), F32),
                pltpu.VMEM((2, 3, dim, CORES * HEAD), BF16),
                pltpu.VMEM((ncp * HEAD, dim), BF16),
                pltpu.VMEM((SLOTS, 2, dim, FB), BF16),
                pltpu.VMEM((SLOTS, FB, dim), BF16),
                pltpu.VMEM((2, dim, tail), BF16),
                pltpu.VMEM((tail, dim), BF16),
                pltpu.SemaphoreType.DMA((n_layers, 3)),
                pltpu.SemaphoreType.DMA((n_layers, 3)),
                pltpu.SemaphoreType.DMA((n_layers, 2)),
                pltpu.SemaphoreType.DMA((n_layers, 2)),
                pltpu.SemaphoreType.DMA((2,)),
                pltpu.SemaphoreType.DMA,
                pltpu.SemaphoreType.DMA((SLOTS,)),
                pltpu.SemaphoreType.DMA,
                pltpu.SemaphoreType.DMA((n_layers, 2)),
            ],
            compiler_params=pltpu.CompilerParams(collective_id=0, has_side_effects=True,
                                                 vmem_limit_bytes=67043328),
        )(x, cos, sin, g1, g2, wq, wk, wv, wo, w1, w3, w2)
        y, kc, vc = _settle(y.reshape(2, rows // 2, dim), kc, vc)
        return y.reshape(rows, dim), kc[:, :, None, :], vc[:, :, None, :]

    return jax.shard_map(body, mesh=mesh, in_specs=(act, P(('req', 'cp'))) + (P(),) * 9,
                         out_specs=(act, cache, cache), check_vma=False)
```

```python
import functools

import jax
import jax.numpy as jnp
from jax import lax
from jax.experimental import pallas as pl
from jax.experimental.pallas import tpu as pltpu
from jax.sharding import PartitionSpec as P

HEAD = 128
F32 = jnp.float32
BF16 = jnp.bfloat16
MESH = pl.DeviceIdType.MESH
CORES = 2
QB = 512
KB = 512
FB = 512
SLOTS = 3
SCALE2 = HEAD ** -0.5 * 1.4426950408889634


def _angles(pos):
    half = HEAD // 2
    inv = 1.0 / (10000.0 ** (jnp.arange(half, dtype=F32) * (2.0 / HEAD)))
    ang = pos.astype(F32)[:, None] * inv
    return jnp.cos(ang), jnp.sin(ang)


def _kernel(ncp, x_ref, cos_ref, sin_ref, g1_ref, g2_ref, wq, wk, wv, wo, w1, w3, w2,
            y_ref, kc_ref, vc_ref,
            x_s, h_s, stage, qkv, o_s, o_stage, m_s, l_s, acc_s, y_acc,
            wqkv_s, wo_s, w13_s, w2_s, w13t_s, w2t_s,
            send_sem, recv_sem, osend_sem, orecv_sem,
            wqkv_sem, wo_sem, wm_sem, wt_sem, out_sem):
    n_layers = wq.shape[0]
    rows, dim = x_ref.shape
    seg = rows // 2
    nseg = 2 * ncp
    seq = nseg * seg
    half_seq = seq // 2
    ff = w1.shape[2]
    nf = ff // FB
    tail = ff - nf * FB
    nchip = ncp // CORES
    last = nchip - 1
    cw = CORES * HEAD
    me = lax.axis_index("cp")
    req = lax.axis_index("req")
    chip, core = me // CORES, me % CORES
    others = (ncp - 1) * seg
    qpasses = [(0, 2)] + [(l, h) for l in range(1, n_layers) for h in range(2)]
    mpasses = [(l, h) for l in range(n_layers - 1) for h in range(2)] + [(n_layers - 1, 2)]
    part = (slice(0, seg), slice(seg, rows), slice(0, rows))

    def chip_at(j):
        off = nchip // 2 + (2 * (j % 2) - 1) * ((j + 1) // 2)
        return lax.rem(chip + off + nchip, nchip)

    def wqkv_copies(p, j):
        slot = (p * nchip + j) % 2 if isinstance(j, int) else lax.rem(p * nchip + j, 2)
        cols = pl.ds(pl.multiple_of(chip_at(j) * cw, cw), cw)
        return [pltpu.make_async_copy(w.at[qpasses[p][0], :, cols], wqkv_s.at[slot, t], wqkv_sem.at[slot])
                for t, w in enumerate((wk, wv, wq))]

    def mlp_copies(p, f, slot):
        l = mpasses[p][0]
        cols = pl.ds(pl.multiple_of(f * FB, FB), FB)
        return [pltpu.make_async_copy(w1.at[l, :, cols], w13_s.at[slot, 0], wm_sem.at[slot]),
                pltpu.make_async_copy(w3.at[l, :, cols], w13_s.at[slot, 1], wm_sem.at[slot]),
                pltpu.make_async_copy(w2.at[l, cols, :], w2_s.at[slot], wm_sem.at[slot])]

    def tail_copies(l):
        cols = pl.ds(nf * FB, tail)
        return [pltpu.make_async_copy(w1.at[l, :, cols], w13t_s.at[0], wt_sem),
                pltpu.make_async_copy(w3.at[l, :, cols], w13t_s.at[1], wt_sem),
                pltpu.make_async_copy(w2.at[l, cols, :], w2t_s, wt_sem)]

    def wo_copies(l):
        return [pltpu.make_async_copy(wo.at[l], wo_s, wo_sem)]

    def start(cs):
        for c in cs:
            c.start()

    def wait(cs):
        for c in cs:
            c.wait()

    def remote(src, dst, ssem, rsem, dev):
        return pltpu.make_async_remote_copy(src_ref=src, dst_ref=dst, send_sem=ssem, recv_sem=rsem,
                                            device_id=(req, dev), device_id_type=MESH)

    def norm(g_ref, l, h):
        blk = 32
        first = part[h].start // blk

        def body(i, _):
            r = pl.ds(pl.multiple_of(i * blk, blk), blk)
            v = x_s[r, :].astype(F32)
            s = lax.rsqrt(jnp.mean(v * v, axis=-1, keepdims=True) + 1e-5)
            h_s[r, :] = (v * s * g_ref[l:l + 1, :].astype(F32)).astype(BF16)
            return 0

        lax.fori_loop(first, part[h].stop // blk, body, 0)

    x_in = pltpu.make_async_copy(x_ref, x_s, out_sem.at[0, 0])
    x_in.start()
    start(wqkv_copies(0, 0))
    start(wqkv_copies(0, 1))
    barrier = pltpu.get_barrier_semaphore()

    def sig(i, _):
        pl.semaphore_signal(barrier, inc=1, device_id=(req, lax.rem(me + 1 + i, ncp)), device_id_type=MESH)
        return 0

    lax.fori_loop(0, ncp - 1, sig, 0)
    x_in.wait()

    def row_of(dev, half):
        r = dev * seg if half == 0 else (nseg - 1 - dev) * seg
        return pl.ds(pl.multiple_of(r, seg), seg)

    A_ALL, B_KV, B_Q = (0, slice(0, 3), 0), (1, slice(0, 2), 1), (1, slice(2, 3), 2)

    def piece(l, j, hh, what):
        half, ts, sem = what
        dev = chip_at(j) * CORES + hh
        return remote(stage.at[j, hh, ts, pl.ds(half * seg, seg), :], qkv.at[l, ts, row_of(me, half), :],
                      send_sem.at[l, sem], recv_sem.at[l, sem], dev)

    def send_chunk(l, j, what):
        for hh in range(CORES):
            piece(l, j, hh, what).start()

    def send_sibling(l, what):
        piece(l, last, 1 - core, what).start()

    def send_all(l, what):
        lax.fori_loop(0, last, lambda j, _: (send_chunk(l, j, what), 0)[1], 0)
        send_sibling(l, what)

    def keep_own(l, half):
        qkv[l, :, row_of(me, half), :] = stage[last, core, :, half * seg:(half + 1) * seg, :]

    def project(p):
        l, h = qpasses[p]
        sl = part[h]
        c, sn = cos_ref[sl, :], sin_ref[sl, :]
        cosv, sinv = jnp.concatenate([c, c], axis=1), jnp.concatenate([-sn, sn], axis=1)

        def body(j, _):
            slot = lax.rem(p * nchip + j, 2)
            wait(wqkv_copies(p, j))
            a = h_s[sl, :]
            for t in range(3):
                r = jnp.dot(a, wqkv_s[slot, t], preferred_element_type=F32)
                for hh in range(CORES):
                    v = r[:, hh * HEAD:(hh + 1) * HEAD]
                    if t != 1:
                        v = v * cosv + pltpu.roll(v, HEAD // 2, 1) * sinv
                    stage[j, hh, t, sl, :] = v.astype(BF16)

            @pl.when(j + 2 < nchip)
            def _():
                start(wqkv_copies(p, j + 2))

            if p + 1 < len(qpasses):
                @pl.when(j + 2 >= nchip)
                def _():
                    start(wqkv_copies(p + 1, j + 2 - nchip))

            if p == 0:
                @pl.when(j == 1)
                def _():
                    pl.semaphore_wait(barrier, ncp - 1)

            @pl.when(j > 0)
            def _():
                send_chunk(l, j - 1, B_Q if h == 1 else A_ALL)
            return 0

        lax.fori_loop(0, nchip, body, 0)
        send_sibling(l, B_Q if h == 1 else A_ALL)
        if h == 1:
            send_all(l, B_KV)
        for half in ((0, 1) if h == 2 else (h,)):
            keep_own(l, half)

    def attend(l, qb, kb, st, masked):
        q = qkv[l, 2, pl.ds(pl.multiple_of(qb * QB, QB), QB), :]
        kr = pl.ds(pl.multiple_of(kb * KB, KB), KB)
        s = lax.dot_general(q, qkv[l, 0, kr, :], (((1,), (1,)), ((), ())), preferred_element_type=F32)
        if masked:
            ri = lax.broadcasted_iota(jnp.int32, (QB, KB), 0)
            ci = lax.broadcasted_iota(jnp.int32, (QB, KB), 1)
            s = jnp.where(ci <= ri, s, -jnp.inf)
        m_old = m_s[st]
        m_new = jnp.maximum(m_old, jnp.max(s, axis=1, keepdims=True))
        mc = m_new * SCALE2
        alpha = jnp.exp2(m_old * SCALE2 - mc)
        ps, tot = [], l_s[st] * alpha
        for c in range(KB // 128):
            p = jnp.exp2(s[:, c * 128:(c + 1) * 128] * SCALE2 - mc)
            tot = tot + p
            ps.append(p.astype(BF16))
        m_s[st] = m_new
        l_s[st] = tot
        pv = jnp.dot(jnp.concatenate(ps, axis=1), qkv[l, 1, kr, :], preferred_element_type=F32)
        acc_s[st] = acc_s[st] * alpha + pv

    def attend_init(st):
        m_s[st] = jnp.full((QB, 128), -jnp.inf, F32)
        l_s[st] = jnp.zeros((QB, 128), F32)
        acc_s[st] = jnp.zeros((QB, HEAD), F32)

    my_cols = pl.ds(pl.multiple_of(me * HEAD, HEAD), HEAD)
    nblk = half_seq // QB

    def finish(l, qb, st, half):
        o = (acc_s[st] / jnp.sum(l_s[st], axis=1, keepdims=True)).astype(BF16)
        o_stage[pl.ds(pl.multiple_of(qb * QB, QB), QB), :] = o
        for i in range(QB // seg):
            s_i = qb * (QB // seg) + i
            dev = s_i if half == 0 else nseg - 1 - s_i

            @pl.when(dev == me)
            def _():
                o_s[l, half * seg:(half + 1) * seg, my_cols] = o[i * seg:(i + 1) * seg]

            @pl.when(dev != me)
            def _():
                remote(o_stage.at[pl.ds(pl.multiple_of(s_i * seg, seg), seg), :],
                       o_s.at[l, pl.ds(half * seg, seg), my_cols],
                       osend_sem.at[l, half], orecv_sem.at[l, half], dev).start()

    def attend_a(l):
        def body(qb, _):
            attend_init(qb)
            lax.fori_loop(0, qb, lambda kb, _: (attend(l, qb, kb, qb, False), 0)[1], 0)
            attend(l, qb, qb, qb, True)
            finish(l, qb, qb, 0)
            return 0

        lax.fori_loop(0, nblk, body, 0)

    def attend_ba(l):
        def body(i, _):
            attend_init(i)
            lax.fori_loop(0, nblk, lambda kb, _: (attend(l, nblk + i, kb, i, False), 0)[1], 0)
            return 0

        lax.fori_loop(0, nblk, body, 0)

    def attend_bb(l):
        def body(i, _):
            qb = nblk + i
            lax.fori_loop(nblk, qb, lambda kb, _: (attend(l, qb, kb, i, False), 0)[1], 0)
            attend(l, qb, qb, i, True)
            finish(l, qb, i, 1)
            return 0

        lax.fori_loop(0, nblk, body, 0)

    def bulk(l, ts, n, ssem, rsem):
        r = qkv.at[l, ts, pl.ds(0, n * seg), :]
        return remote(r, r, ssem, rsem, me)

    def recv(l, what):
        bulk(l, what[1], ncp - 1, send_sem.at[l, what[2]], recv_sem.at[l, what[2]]).wait_recv()

    def sent(l, half):
        for _, ts, sem in ((A_ALL,) if half == 0 else (B_Q, B_KV)):
            bulk(l, ts, ncp - 1, send_sem.at[l, sem], recv_sem.at[l, sem]).wait_send()

    def o_recv(l, half):
        bulk(l, slice(0, 1), ncp - 1, osend_sem.at[l, half], orecv_sem.at[l, half]).wait_recv()

    def o_sent(l, half):
        bulk(l, slice(0, 1), ncp - 1, osend_sem.at[l, half], orecv_sem.at[l, half]).wait_send()

    def mlp_step(a, w13, w2c):
        g = jnp.dot(a, w13[0], preferred_element_type=F32)
        u = jnp.dot(a, w13[1], preferred_element_type=F32)
        u = (g * (1.0 / (1.0 + jnp.exp(-g))) * u).astype(BF16)
        return jnp.dot(u, w2c, preferred_element_type=F32)

    def dense(p):
        l, h = mpasses[p]
        sl = part[h]
        reload = p + 1 < len(mpasses) and mpasses[p + 1][0] != l
        first = p == 0 or mpasses[p - 1][0] != l
        if first:
            wait(wo_copies(l))

        def out_proj(c, _):
            cols = pl.ds(pl.multiple_of(c * FB, FB), FB)
            x_s[sl, cols] = (x_s[sl, cols].astype(F32)
                             + jnp.dot(o_s[l, sl, :], wo_s[:, cols], preferred_element_type=F32)).astype(BF16)
            return 0

        lax.fori_loop(0, dim // FB, out_proj, 0)
        if reload:
            start(wo_copies(l + 1))
        norm(g2_ref, l, h)
        if first:
            wait(tail_copies(l))
        y_acc[sl, :] = mlp_step(h_s[sl, :], w13t_s, w2t_s[...])
        if reload:
            start(tail_copies(l + 1))

        def body(f, _):
            slot = lax.rem(p * nf + f, SLOTS)
            wait(mlp_copies(p, f, slot))
            y_acc[sl, :] += mlp_step(h_s[sl, :], w13_s.at[slot], w2_s[slot])

            @pl.when(f + SLOTS < nf)
            def _():
                start(mlp_copies(p, f + SLOTS, slot))

            if p + 1 < len(mpasses):
                @pl.when(f + SLOTS >= nf)
                def _():
                    start(mlp_copies(p + 1, f + SLOTS - nf, slot))

            return 0

        lax.fori_loop(0, nf, body, 0)
        x_s[sl, :] = (x_s[sl, :].astype(F32) + y_acc[sl, :]).astype(BF16)

    norm(g1_ref, 0, 2)
    project(0)
    send_all(0, B_Q)
    start(wo_copies(0))
    start(tail_copies(0))
    for f in range(SLOTS):
        start(mlp_copies(0, f, f))
    outs = []
    for l in range(n_layers):
        if l > 0:
            o_sent(l - 1, 0)
        recv(l, A_ALL)
        attend_a(l)
        recv(l, B_Q)
        attend_ba(l)
        more = l + 1 < n_layers
        if more:
            o_recv(l, 0)
            if l == 0:
                send_all(l, B_KV)
            dense(2 * l)
            norm(g1_ref, l + 1, 0)
        if l > 0:
            o_sent(l - 1, 1)
        recv(l, B_KV)
        for i, c in enumerate((kc_ref, vc_ref)):
            cp = pltpu.make_async_copy(qkv.at[l, i], c.at[l], out_sem.at[l, i])
            cp.start()
            outs.append(cp)
        attend_bb(l)
        sent(l, 0)
        if more:
            project(2 * l + 1)
            o_recv(l, 1)
            dense(2 * l + 1)
            norm(g1_ref, l + 1, 1)
            sent(l, 1)
            project(2 * l + 2)
        else:
            sent(l, 1)
            o_recv(l, 0)
            o_recv(l, 1)
            dense(2 * l)
            o_sent(l, 0)
            o_sent(l, 1)
    wait(outs)
    out = pltpu.make_async_copy(x_s, y_ref, out_sem.at[0, 0])
    out.start()
    out.wait()


def _copy_kernel(*refs):
    n = len(refs) // 3
    ins, outs, bufs, rsem, wsem = refs[:n], refs[n:2 * n], refs[2 * n:3 * n], refs[3 * n], refs[3 * n + 1]
    jobs = []
    for a, b, buf in zip(ins, outs, bufs):
        for i in range(a.shape[0]):
            jobs.append((pltpu.make_async_copy(a.at[i], buf.at[i], rsem.at[len(jobs)]),
                         pltpu.make_async_copy(buf.at[i], b.at[i], wsem.at[len(jobs)])))
    for r, _ in jobs:
        r.start()
    for r, w in jobs:
        r.wait()
        w.start()
    for _, w in jobs:
        w.wait()


def _settle(*arrays):
    hbm = pl.BlockSpec(memory_space=pl.ANY)
    n = sum(a.shape[0] for a in arrays)
    return pl.pallas_call(
        _copy_kernel,
        out_shape=tuple(jax.ShapeDtypeStruct(a.shape, a.dtype) for a in arrays),
        in_specs=[hbm] * len(arrays),
        out_specs=(hbm,) * len(arrays),
        scratch_shapes=[pltpu.VMEM(a.shape, a.dtype) for a in arrays]
        + [pltpu.SemaphoreType.DMA((n,)), pltpu.SemaphoreType.DMA((n,))],
    )(*arrays)


def solution(mesh):
    ncp = mesh.shape['cp']
    act = P(('req', 'cp'), None)
    cache = P(None, 'req', 'cp', None)

    def body(x, pos, g1, g2, wq, wk, wv, wo, w1, w3, w2):
        rows, dim = x.shape
        n_layers, _, ff = w1.shape
        seq = rows * ncp
        tail = ff % FB
        nchip = ncp // CORES
        cos, sin = _angles(pos)
        vm = pl.BlockSpec(memory_space=pltpu.VMEM)
        hbm = pl.BlockSpec(memory_space=pl.ANY)
        nb = seq // 2 // QB
        y, kc, vc = pl.pallas_call(
            functools.partial(_kernel, ncp),
            out_shape=(jax.ShapeDtypeStruct((rows, dim), BF16),
                       jax.ShapeDtypeStruct((n_layers, seq, HEAD), BF16),
                       jax.ShapeDtypeStruct((n_layers, seq, HEAD), BF16)),
            in_specs=[hbm] + [vm] * 4 + [hbm] * 7,
            out_specs=(hbm,) * 3,
            scratch_shapes=[
                pltpu.VMEM((rows, dim), BF16),
                pltpu.VMEM((rows, dim), BF16),
                pltpu.VMEM((nchip, CORES, 3, rows, HEAD), BF16),
                pltpu.VMEM((n_layers, 3, seq, HEAD), BF16),
                pltpu.VMEM((n_layers, rows, ncp * HEAD), BF16),
                pltpu.VMEM((seq, HEAD), BF16),
                pltpu.VMEM((nb, QB, 128), F32),
                pltpu.VMEM((nb, QB, 128), F32),
                pltpu.VMEM((nb, QB, HEAD), F32),
                pltpu.VMEM((rows, dim), F32),
                pltpu.VMEM((2, 3, dim, CORES * HEAD), BF16),
                pltpu.VMEM((ncp * HEAD, dim), BF16),
                pltpu.VMEM((SLOTS, 2, dim, FB), BF16),
                pltpu.VMEM((SLOTS, FB, dim), BF16),
                pltpu.VMEM((2, dim, tail), BF16),
                pltpu.VMEM((tail, dim), BF16),
                pltpu.SemaphoreType.DMA((n_layers, 3)),
                pltpu.SemaphoreType.DMA((n_layers, 3)),
                pltpu.SemaphoreType.DMA((n_layers, 2)),
                pltpu.SemaphoreType.DMA((n_layers, 2)),
                pltpu.SemaphoreType.DMA((2,)),
                pltpu.SemaphoreType.DMA,
                pltpu.SemaphoreType.DMA((SLOTS,)),
                pltpu.SemaphoreType.DMA,
                pltpu.SemaphoreType.DMA((n_layers, 2)),
            ],
            compiler_params=pltpu.CompilerParams(collective_id=0, has_side_effects=True,
                                                 vmem_limit_bytes=67043328),
        )(x, cos, sin, g1, g2, wq, wk, wv, wo, w1, w3, w2)
        y, kc, vc = _settle(y.reshape(2, rows // 2, dim), kc, vc)
        return y.reshape(rows, dim), kc[:, :, None, :], vc[:, :, None, :]

    return jax.shard_map(body, mesh=mesh, in_specs=(act, P(('req', 'cp'))) + (P(),) * 9,
                         out_specs=(act, cache, cache), check_vma=False)
```
